32 devices in a mesh: data: 2 (over x), col: 4 (over z), row: 4 (over y, core).
Axes of the slice: x: 2, y: 2, z: 4, core: 2. Of those that a mesh axis runs over, the one named last changes fastest.
Arguments:
- pair_rep: bfloat16 [768, 384, 64], P(('data', 'row'), 'col'), parts along dimension 0
- res_mask: int32 [768], P('data'), parts along dimension 0
- ln_gamma: float32 [64], replicated
- ln_beta: float32 [64], replicated
- w_q: bfloat16 [64, 64], replicated
- w_k: bfloat16 [64, 64], replicated
- w_v: bfloat16 [64, 64], replicated
- w_b: bfloat16 [64, 4], replicated
- w_g: bfloat16 [64, 64], replicated
- w_o: bfloat16 [64, 64], replicated
Outputs:
- output: bfloat16 [768, 384, 64], P(('data', 'row'), 'col'), parts along dimension 0
There are 2 independent parts. The reference program is written for one: setup_inputs(seed, part) draws one part's arguments, and reference() takes and returns one part's arrays. A program takes and returns all parts, laid end to end along the dimension named above; an argument that names none is the same for every part.
All inputs are finite; a program needn't handle non-finite values.
Results may differ from the reference program's by a relative error of at most 0.00624027.
Values are sent between devices in bfloat16 or wider.
A program may use at most 1 GiB of HBM per device.

```python
import math
import jax
import jax.numpy as jnp
from jax import lax

N = 384
C_Z = 64
HEADS = 4
HEAD = 16

PROJ = HEADS * HEAD
Q_SCALE = 1.0 / math.sqrt(HEAD)
LN_EPS = 1e-5
MASK_FILL = -1e9
OUT_GAIN = 0.35 * math.sqrt(N / PROJ)


def setup_inputs(seed: int = 0, part: int = 0) -> dict:
    base_key = jax.random.key(seed)
    part_key = jax.random.fold_in(base_key, part)
    key_pair, key_len = jax.random.split(part_key, 2)
    pair_rep = jax.random.normal(key_pair, (N, N, C_Z), jnp.float32).astype(jnp.bfloat16)
    pad_len = jax.random.randint(key_len, (), N // 16, N // 4 + 1)
    res_mask = (jnp.arange(N) < N - pad_len).astype(jnp.int32)
    weight_keys = jax.random.split(base_key, 8)
    in_scale = 1.0 / math.sqrt(C_Z)
    ln_gamma = jax.random.uniform(weight_keys[0], (C_Z,), jnp.float32, 0.5, 1.5)
    ln_beta = 0.1 * jax.random.normal(weight_keys[1], (C_Z,), jnp.float32)
    w_q = (in_scale * jax.random.normal(weight_keys[2], (C_Z, PROJ), jnp.float32)).astype(jnp.bfloat16)
    w_k = (in_scale * jax.random.normal(weight_keys[3], (C_Z, PROJ), jnp.float32)).astype(jnp.bfloat16)
    w_v = (in_scale * jax.random.normal(weight_keys[4], (C_Z, PROJ), jnp.float32)).astype(jnp.bfloat16)
    w_b = (in_scale * jax.random.normal(weight_keys[5], (C_Z, HEADS), jnp.float32)).astype(jnp.bfloat16)
    w_g = (in_scale * jax.random.normal(weight_keys[6], (C_Z, PROJ), jnp.float32)).astype(jnp.bfloat16)
    w_o = (OUT_GAIN * jax.random.normal(weight_keys[7], (PROJ, C_Z), jnp.float32)).astype(jnp.bfloat16)
    return {'pair_rep': pair_rep, 'res_mask': res_mask, 'ln_gamma': ln_gamma, 'ln_beta': ln_beta, 'w_q': w_q, 'w_k': w_k, 'w_v': w_v, 'w_b': w_b, 'w_g': w_g, 'w_o': w_o}


def reference(pair_rep, res_mask, ln_gamma, ln_beta, w_q, w_k, w_v, w_b, w_g, w_o):
    pair_f32 = pair_rep.astype(jnp.float32)
    mean = jnp.mean(pair_f32, axis=-1, keepdims=True)
    centred = pair_f32 - mean
    variance = jnp.mean(centred * centred, axis=-1, keepdims=True)
    normed = (centred * lax.rsqrt(variance + LN_EPS) * ln_gamma + ln_beta).astype(jnp.bfloat16)
    bias = jnp.dot(normed.reshape(N * N, C_Z), w_b, preferred_element_type=jnp.float32).astype(jnp.bfloat16).reshape(N, N, HEADS)
    key_fill = jnp.where(res_mask > 0, 0.0, MASK_FILL).astype(jnp.float32)
    bias_ik = jnp.transpose(bias, (1, 0, 2)).astype(jnp.float32) + key_fill[None, :, None]

    def one_column(col_args):
        a_col, z_col = col_args
        query = (jnp.dot(a_col, w_q, preferred_element_type=jnp.float32) * Q_SCALE).astype(jnp.bfloat16).reshape(N, HEADS, HEAD)
        keys = jnp.dot(a_col, w_k, preferred_element_type=jnp.float32).astype(jnp.bfloat16).reshape(N, HEADS, HEAD)
        values = jnp.dot(a_col, w_v, preferred_element_type=jnp.float32).astype(jnp.bfloat16).reshape(N, HEADS, HEAD)
        gate = jax.nn.sigmoid(jnp.dot(a_col, w_g, preferred_element_type=jnp.float32))
        logits = jnp.einsum('ihd,khd->ikh', query.astype(jnp.float32), keys.astype(jnp.float32)) + bias_ik
        attn_prob = jax.nn.softmax(logits, axis=1)
        attended = jnp.einsum('ikh,khd->ihd', attn_prob, values.astype(jnp.float32)).reshape(N, PROJ)
        gated = (gate * attended).astype(jnp.bfloat16)
        return (z_col.astype(jnp.float32) + jnp.dot(gated, w_o, preferred_element_type=jnp.float32)).astype(jnp.bfloat16)

    out_cols = lax.map(one_column, (jnp.transpose(normed, (1, 0, 2)), jnp.transpose(pair_rep, (1, 0, 2))))
    return jnp.transpose(out_cols, (1, 0, 2))
```

```python
import functools
import math

import jax
import jax.numpy as jnp
from jax import lax
from jax.experimental import pallas as pl
from jax.experimental.pallas import tpu as pltpu
from jax.sharding import PartitionSpec as P

LN_EPS = 1e-5
MASK_FILL = -1e9
LOG2E = math.log2(math.e)
HEADS = 4
HD = 16
C = 64
NB = 96
NK = 384
NQ = 192
PAIRS = 24
CHUNK = 4
NCH = PAIRS // CHUNK
MESH = pl.DeviceIdType.MESH
F32 = jnp.float32
BF16 = jnp.bfloat16


def dot(a, b, ca=1, cb=0):
    return lax.dot_general(a, b, (((ca,), (cb,)), ((), ())), preferred_element_type=F32)


def kernel(a_ref, bt_ref, fill_ref, wkt_ref, wv_ref, wqg_ref, g_ref,
           a_all, bias_in, bias_f, kbd, vbd, p_ref, g_send, g_recv,
           a_ssem, a_rsem, b_ssem, b_rsem, f_ssem, g_ssem, g_rsem):
    col = lax.axis_index("col")
    row = lax.axis_index("row")
    y, s = row // 2, lax.rem(row, 2)
    u_own = lax.rem(col, 2)
    y_tgt = col // 2
    partner = y * 2 + (1 - s)
    across = (1 - y) * 2 + s
    cross = (1 - y) * 2 + (1 - s)
    peers = (partner, across, cross)

    barrier = pltpu.get_barrier_semaphore()
    for r in peers:
        pl.semaphore_signal(barrier, inc=1, device_id={"row": r}, device_id_type=MESH)
    for d in range(1, 4):
        pl.semaphore_signal(barrier, inc=1, device_id={"col": lax.rem(col + d, 4)}, device_id_type=MESH)

    a_all[:, pl.ds(pl.multiple_of(row * NB, NB), NB), :] = a_ref[pl.ds(s * PAIRS, PAIRS)]
    kbd[...] = jnp.zeros_like(kbd)
    pl.semaphore_wait(barrier, 6)

    def bias_copy(src, u, r, ssem, dev):
        return pltpu.make_async_remote_copy(
            src_ref=src, dst_ref=bias_in.at[u, r], send_sem=ssem, recv_sem=b_rsem.at[u, r],
            device_id=dev, device_id_type=MESH)

    def bias_wait(u, r):
        bias_copy(bias_in.at[u, r], u, r, b_ssem.at[0], {"row": partner}).wait_recv()

    is_src = y_tgt == y

    @pl.when(jnp.logical_not(is_src))
    def _():
        bias_copy(bt_ref, u_own, row, b_ssem.at[0], {"row": across}).start()

    def a_copy(slot, q, r):
        s_d = lax.rem(r, 2)
        return pltpu.make_async_remote_copy(
            src_ref=a_ref.at[pl.ds(s_d * PAIRS + q * CHUNK, CHUNK)],
            dst_ref=a_all.at[pl.ds(q * CHUNK, CHUNK), pl.ds(pl.multiple_of(row * NB, NB), NB)],
            send_sem=a_ssem.at[slot, q], recv_sem=a_rsem.at[slot, q],
            device_id={"row": r}, device_id_type=MESH)

    def a_wait_recv(slot, q, r):
        pltpu.make_async_remote_copy(
            src_ref=a_ref.at[pl.ds(0, CHUNK)],
            dst_ref=a_all.at[pl.ds(q * CHUNK, CHUNK), pl.ds(pl.multiple_of(r * NB, NB), NB)],
            send_sem=a_ssem.at[slot, q], recv_sem=a_rsem.at[slot, q],
            device_id={"row": r}, device_id_type=MESH).wait_recv()

    for q in range(NCH):
        for slot, r in enumerate(peers):
            a_copy(slot, q, r).start()

    @pl.when(is_src)
    def _():
        bias_in[u_own, row] = bt_ref[...]
        for d in range(1, 4):
            bias_copy(bt_ref, u_own, row, b_ssem.at[d], {"col": lax.rem(col + d, 4)}).start()
        bias_wait(u_own, across)
        for d in range(1, 4):
            bias_copy(bias_in.at[u_own, across], u_own, across, b_ssem.at[3 + d],
                      {"col": lax.rem(col + d, 4)}).start()
        bias_wait(1 - u_own, row)
        bias_wait(1 - u_own, across)

    @pl.when(jnp.logical_not(is_src))
    def _():
        for u in range(2):
            bias_wait(u, row)
            bias_wait(u, across)

    for u in range(2):
        for i, r in enumerate((row, across)):
            bias_copy(bias_in.at[u, r], u, r, f_ssem.at[u, i], {"row": partner}).start()
    for u in range(2):
        for r in (partner, cross):
            bias_wait(u, r)

    lane = lax.broadcasted_iota(jnp.int32, (NB, 128), 1)
    for u in range(2):
        for h in range(HEADS):
            t = [bias_in[u, r, :, h * 128:(h + 1) * 128].astype(F32) for r in range(4)]
            parts = (jnp.where(lane < 96, t[0], t[1]), jnp.where(lane < 64, t[1], t[2]),
                     jnp.where(lane < 32, t[2], t[3]))
            for i, part in enumerate(parts):
                sl = slice(i * 128, (i + 1) * 128)
                bias_f[h, u * NB:(u + 1) * NB, sl] = (part + fill_ref[:, sl]) * LOG2E

    hid = lax.broadcasted_iota(jnp.int32, (NK, C), 1) // HD
    hid_q = lax.broadcasted_iota(jnp.int32, (NQ, C), 1) // HD

    def pair(p):
        x = a_all[p]
        xq = a_all[p, pl.ds(pl.multiple_of(y * NQ, NQ), NQ), :]
        qg = dot(xq, wqg_ref[...])
        q2 = (qg[:, :128] * (1.0 / math.sqrt(HD))).astype(BF16)
        v2 = dot(x, wv_ref[...]).astype(BF16)
        kt = dot(wkt_ref[...], x, 1, 1).astype(BF16)
        gated = []
        for jj in range(2):
            q_j = q2[:, jj * C:(jj + 1) * C]
            v_j = v2[:, jj * C:(jj + 1) * C]
            for h in range(HEADS):
                kbd[h * HD:(h + 1) * HD, h * NK:(h + 1) * NK] = kt[jj * C + h * HD:jj * C + (h + 1) * HD, :]
                vbd[h * NK:(h + 1) * NK, :] = jnp.where(hid == h, v_j, jnp.zeros_like(v_j))
            inv = []
            for hp in range(2):
                logits = dot(q_j, kbd[:, hp * 2 * NK:(hp + 1) * 2 * NK])
                for hh in range(2):
                    h = hp * 2 + hh
                    t = logits[:, hh * NK:(hh + 1) * NK] * LOG2E + bias_f[h]
                    m = jnp.max(t, axis=1, keepdims=True)
                    e = jnp.exp2(t - m)
                    inv.append(1.0 / jnp.sum(e, axis=1, keepdims=True))
                    p_ref[:, h * NK:(h + 1) * NK] = e.astype(BF16)
            o = dot(p_ref[...], vbd[...])
            scale = jnp.where(hid_q == 0, inv[0], jnp.where(hid_q == 1, inv[1], jnp.where(hid_q == 2, inv[2], inv[3])))
            gate = jax.nn.sigmoid(qg[:, 128 + jj * C:128 + (jj + 1) * C])
            gated.append(gate * (o * scale))
        return jnp.concatenate(gated, axis=1).astype(BF16)

    def g_copy(q):
        return pltpu.make_async_remote_copy(
            src_ref=g_send.at[pl.ds(q * CHUNK, CHUNK)], dst_ref=g_recv.at[pl.ds(q * CHUNK, CHUNK)],
            send_sem=g_ssem.at[q], recv_sem=g_rsem.at[q], device_id={"row": partner}, device_id_type=MESH)

    @pl.loop(0, NCH)
    def _(q):
        for slot, r in enumerate(peers):
            a_wait_recv(slot, q, r)

        @pl.loop(0, CHUNK)
        def _(i):
            p = q * CHUNK + i
            res = pair(p)
            g_ref[s * PAIRS + p] = jnp.where(s == 0, res[:NB], res[NB:])
            g_send[p] = jnp.where(s == 0, res[NB:], res[:NB])

        g_copy(q).start()

    for q in range(NCH):
        g_copy(q).wait_recv()
    g_ref[pl.ds((1 - s) * PAIRS, PAIRS)] = g_recv[...]
    for q in range(NCH):
        g_copy(q).wait_send()
        for slot, r in enumerate(peers):
            a_copy(slot, q, r).wait_send()

    @pl.when(is_src)
    def _():
        for d in range(1, 7):
            bias_copy(bt_ref, u_own, row, b_ssem.at[d], {"row": partner}).wait_send()

    @pl.when(jnp.logical_not(is_src))
    def _():
        bias_copy(bt_ref, u_own, row, b_ssem.at[0], {"row": across}).wait_send()

    for u in range(2):
        for i, r in enumerate((row, across)):
            bias_copy(bias_in.at[u, r], u, r, f_ssem.at[u, i], {"row": partner}).wait_send()


def attend(a2, bt, fill, wkt, wv, wqg):
    vm = pl.BlockSpec(memory_space=pltpu.VMEM)
    dma = pltpu.SemaphoreType.DMA
    return pl.pallas_call(
        kernel,
        out_shape=jax.ShapeDtypeStruct((2 * PAIRS, NB, 128), BF16),
        in_specs=[vm] * 6,
        out_specs=vm,
        scratch_shapes=[
            pltpu.VMEM((PAIRS, NK, 128), BF16),
            pltpu.VMEM((2, 4, NB, HEADS * 128), BF16),
            pltpu.VMEM((HEADS, NQ, NK), F32),
            pltpu.VMEM((C, HEADS * NK), BF16),
            pltpu.VMEM((HEADS * NK, C), BF16),
            pltpu.VMEM((NQ, HEADS * NK), BF16),
            pltpu.VMEM((PAIRS, NB, 128), BF16),
            pltpu.VMEM((PAIRS, NB, 128), BF16),
            dma((3, NCH)), dma((3, NCH)), dma((7,)), dma((2, 4)), dma((2, 2)), dma((NCH,)), dma((NCH,)),
        ],
        compiler_params=pltpu.CompilerParams(collective_id=0, has_side_effects=True, vmem_limit_bytes=56 * 2**20),
        name="attend",
    )(a2, bt, fill, wkt, wv, wqg)


def blockdiag2(w):
    z = jnp.zeros_like(w)
    return jnp.concatenate([jnp.concatenate([w, z], 1), jnp.concatenate([z, w], 1)], 0)


def solution(mesh):
    def body(pair_tile, res_mask, ln_gamma, ln_beta, w_q, w_k, w_v, w_b, w_g, w_o):
        row = lax.axis_index("row")
        pair_f32 = pair_tile.astype(F32)
        mean = jnp.mean(pair_f32, axis=-1, keepdims=True)
        centred = pair_f32 - mean
        variance = jnp.mean(centred * centred, axis=-1, keepdims=True)
        normed = (centred * lax.rsqrt(variance + LN_EPS) * ln_gamma + ln_beta).astype(BF16)
        a2 = jnp.transpose(normed.reshape(NB, NB // 2, 128), (1, 0, 2))
        bias = jnp.einsum("kic,ch->ihk", normed, w_b, preferred_element_type=F32).astype(BF16)
        bias = jnp.pad(bias, ((0, 0), (0, 0), (0, 128 - NB)))
        bias = jnp.roll(bias, lax.rem(row * NB, 128), axis=2).reshape(NB, HEADS * 128)
        fill = jnp.where(res_mask > 0, 0.0, MASK_FILL).astype(F32)[None, :]
        wqg = jnp.concatenate([blockdiag2(w_q), blockdiag2(w_g)], 1)
        gated = attend(a2, bias, fill, blockdiag2(w_k.T), blockdiag2(w_v), wqg)
        gated = jnp.transpose(gated, (1, 0, 2)).reshape(NB, NB, C)
        update = jnp.einsum("ijd,dc->ijc", gated, w_o, preferred_element_type=F32)
        return (pair_f32 + update).astype(BF16)

    tile_spec = P(("data", "row"), "col", None)
    return jax.shard_map(body, mesh=mesh, in_specs=(tile_spec, P("data"), P(), P(), P(), P(), P(), P(), P(), P()),
                         out_specs=tile_spec, check_vma=False)
```

```python
import math

import jax
import jax.numpy as jnp
from jax import lax
from jax.experimental import pallas as pl
from jax.experimental.pallas import tpu as pltpu
from jax.sharding import PartitionSpec as P

LN_EPS = 1e-5
MASK_FILL = -1e9
LOG2E = math.log2(math.e)
HEADS = 4
HD = 16
C = 64
NB = 96
NK = 384
PAIRS = 24
CHUNK = 4
NCH = PAIRS // CHUNK
L = 128
MESH = pl.DeviceIdType.MESH
F32 = jnp.float32
BF16 = jnp.bfloat16


def dot(a, b, ca=1, cb=0):
    return lax.dot_general(a, b, (((ca,), (cb,)), ((), ())), preferred_element_type=F32)


def blockdiag2(w):
    z = jnp.zeros_like(w)
    return jnp.concatenate([jnp.concatenate([w, z], 1), jnp.concatenate([z, w], 1)], 0)


def transposed(w):
    return jnp.transpose(w.astype(F32)).astype(BF16)


def down(v, n):
    return jnp.transpose(jnp.broadcast_to(v.reshape(1, n), (L, n)))


def kernel(z_ref, mask_ref, gam_ref, bet_ref, wq_ref, wk_ref, wv_ref, wbt_ref, wg_ref, wo_ref, out_ref,
           t_sc, b_sc, a_own, a_all, b_own, bias_in, bias_f, qbd, g_send, g_recv, gf, wk2, wv2, wqg2, wo2,
           a_ssem, a_rsem, b1_ssem, b_ssem, b_rsem, f_ssem, g_ssem, g_rsem):
    col = lax.axis_index("col")
    row = lax.axis_index("row")
    y, s = row // 2, lax.rem(row, 2)
    partner = y * 2 + (1 - s)
    across = (1 - y) * 2 + s
    cross = (1 - y) * 2 + (1 - s)
    peers = (partner, across, cross)

    barrier = pltpu.get_barrier_semaphore()
    for r in peers:
        pl.semaphore_signal(barrier, inc=1, device_id={"row": r}, device_id_type=MESH)

    @pl.when(col > 0)
    def _():
        pl.semaphore_signal(barrier, inc=1, device_id={"col": col - 1}, device_id_type=MESH)

    @pl.when(col < 3)
    def _():
        pl.semaphore_signal(barrier, inc=1, device_id={"col": col + 1}, device_id_type=MESH)

    gam = down(gam_ref[...], C)[:, :NB]
    bet = down(bet_ref[...], C)[:, :NB]
    wbt = wbt_ref[...]

    @pl.loop(0, NB, unroll=4)
    def _(i):
        z = z_ref[i].astype(F32)
        mean = jnp.sum(z, axis=0, keepdims=True) * (1.0 / C)
        cen = z - mean
        var = jnp.sum(cen * cen, axis=0, keepdims=True) * (1.0 / C)
        a = cen * lax.rsqrt(var + LN_EPS) * gam + bet
        b_sc[i, :HEADS, :NB] = dot(wbt, a.astype(BF16))
        at = jnp.transpose(a)
        for half in range(2):
            o = half * 48
            t_sc[pl.ds(pl.multiple_of(i * 48 + half * PAIRS, 8), PAIRS), :] = jnp.concatenate(
                [at[o:o + PAIRS], at[o + PAIRS:o + 2 * PAIRS]], axis=1)

    @pl.loop(0, 2 * PAIRS, unroll=4)
    def _(n):
        a_own[n] = t_sc[pl.ds(n, NB, stride=2 * PAIRS), :].astype(BF16)

    lane = lax.broadcasted_iota(jnp.int32, (NB, L), 1)
    bh = [b_sc.reshape(NB * 8, L)[pl.ds(h, NB, stride=8), :] for h in range(HEADS)]
    for g in range(3):
        b_own[g] = jnp.where(lane < NB, bh[g], pltpu.roll(bh[3], NB - 32 * g, 1)).astype(BF16)

    wk2[...] = blockdiag2(wk_ref[...])
    wv2[...] = blockdiag2(transposed(wv_ref[...]))
    wqg2[:L] = blockdiag2(transposed(wq_ref[...]))
    wqg2[L:] = blockdiag2(transposed(wg_ref[...]))
    wo2[...] = blockdiag2(transposed(wo_ref[...]))
    qbd[...] = jnp.zeros_like(qbd)
    gf[...] = jnp.zeros_like(gf)
    a_all[:, NK:, :] = jnp.zeros((PAIRS, 32, L), BF16)
    a_all[:, pl.ds(pl.multiple_of(row * NB, NB), NB), :] = a_own[pl.ds(s * PAIRS, PAIRS)]

    pl.semaphore_wait(barrier, 3 + jnp.where(col > 0, 1, 0) + jnp.where(col < 3, 1, 0))

    def bias_copy(src, u, r, ssem, dev):
        return pltpu.make_async_remote_copy(
            src_ref=src, dst_ref=bias_in.at[u, r], send_sem=ssem, recv_sem=b_rsem.at[u, r],
            device_id=dev, device_id_type=MESH)

    def bias_wait(u, r):
        bias_copy(bias_in.at[u, r], u, r, b1_ssem, {"row": partner}).wait_recv()

    y_tgt = col // 2
    u_own = lax.rem(col, 2)
    is_src = y_tgt == y

    @pl.when(jnp.logical_not(is_src))
    def _():
        bias_copy(b_own, u_own, row, b1_ssem, {"row": across}).start()

    def a_copy(slot, q, r):
        s_d = lax.rem(r, 2)
        return pltpu.make_async_remote_copy(
            src_ref=a_own.at[pl.ds(s_d * PAIRS + q * CHUNK, CHUNK)],
            dst_ref=a_all.at[pl.ds(q * CHUNK, CHUNK), pl.ds(pl.multiple_of(row * NB, NB), NB)],
            send_sem=a_ssem.at[slot, q], recv_sem=a_rsem.at[slot, q],
            device_id={"row": r}, device_id_type=MESH)

    def a_wait_recv(slot, q, r):
        pltpu.make_async_remote_copy(
            src_ref=a_own.at[pl.ds(0, CHUNK)],
            dst_ref=a_all.at[pl.ds(q * CHUNK, CHUNK), pl.ds(pl.multiple_of(r * NB, NB), NB)],
            send_sem=a_ssem.at[slot, q], recv_sem=a_rsem.at[slot, q],
            device_id={"row": r}, device_id_type=MESH).wait_recv()

    for q in range(NCH):
        for slot, r in enumerate(peers):
            a_copy(slot, q, r).start()

    mine = (row, across)

    def right(u, i):
        return bias_copy(bias_in.at[u, mine[i]], u, mine[i], b_ssem.at[u, i, 0], {"col": jnp.minimum(col + 1, 3)})

    def left(u, i):
        return bias_copy(bias_in.at[u, mine[i]], u, mine[i], b_ssem.at[u, i, 1], {"col": jnp.maximum(col - 1, 0)})

    def to_partner(u, i):
        return bias_copy(bias_in.at[u, mine[i]], u, mine[i], f_ssem.at[u, i], {"row": partner})

    def sends_right(u):
        return jnp.logical_and(col >= 2 * y + u, col < 3)

    def sends_left(u):
        return jnp.logical_and(col <= 2 * y + u, col > 0)

    @pl.when(is_src)
    def _():
        bias_in[u_own, row] = b_own[...]

    for i in range(2):
        for u in range(2):
            own = jnp.logical_and(is_src, u_own == u)
            if i == 0:
                @pl.when(jnp.logical_not(own))
                def _(u=u, i=i):
                    bias_wait(u, mine[i])
            else:
                bias_wait(u, mine[i])

            @pl.when(sends_right(u))
            def _(u=u, i=i):
                right(u, i).start()

            @pl.when(sends_left(u))
            def _(u=u, i=i):
                left(u, i).start()

            to_partner(u, i).start()

    for u in range(2):
        for r in (partner, cross):
            bias_wait(u, r)

    fill = down(jnp.where(mask_ref[...] > 0, 0.0, MASK_FILL).astype(F32), NK)
    for r in range(4):
        for u in range(2):
            for g in range(3):
                sl = slice(r * NB, (r + 1) * NB)
                bias_f[u, g, sl, :] = (bias_in[u, r, g].astype(F32) + fill[sl]) * LOG2E

    lane16 = lax.broadcasted_iota(jnp.int32, (HD, L), 1)

    def pair(p):
        x = a_all[p, :NK, :]
        k2 = dot(x, wk2[...]).astype(BF16)
        vt = dot(wv2[...], x, 1, 1).astype(BF16)
        gate = []
        for u in range(2):
            xu = a_all[p, pl.ds(pl.multiple_of((2 * y + u) * NB, NB), L), :]
            qg = dot(wqg2[...], xu, 1, 1)
            qt = qg[:L] * (1.0 / math.sqrt(HD))
            gate.append(jax.nn.sigmoid(qg[L:]))
            for t in range(2):
                q3 = qt[t * C + 48:t * C + 64]
                for g in range(3):
                    o = (g * 2 + u) * L
                    qgh = qt[t * C + g * HD:t * C + (g + 1) * HD]
                    qbd[t, t * C + g * HD:t * C + (g + 1) * HD, o:o + L] = jnp.where(lane16 < NB, qgh, 0.0).astype(BF16)
                    qbd[t, t * C + 48:t * C + 64, o:o + L] = jnp.where(
                        lane16 < NB, 0.0, pltpu.roll(q3, NB - 32 * g, 1)).astype(BF16)
        att = [[], []]
        for t in range(2):
            o_t = []
            for g in range(3):
                logits = dot(k2, qbd[t, :, g * 2 * L:(g + 1) * 2 * L])
                lt = logits * LOG2E + jnp.concatenate([bias_f[0, g], bias_f[1, g]], axis=1)
                m = jnp.max(lt, axis=0, keepdims=True)
                e = jnp.exp2(lt - m)
                inv = 1.0 / jnp.sum(e, axis=0, keepdims=True)
                vg = jnp.concatenate([vt[t * C + g * HD:t * C + (g + 1) * HD], vt[t * C + 48:t * C + 64]], axis=0)
                o_t.append(dot(vg, e.astype(BF16)) * inv)
            for u in range(2):
                parts = [o_t[g][:HD, u * L:(u + 1) * L] for g in range(3)]
                last = [pltpu.roll(o_t[g][HD:, u * L:(u + 1) * L], 32 + 32 * g, 1) for g in range(3)]
                parts.append(jnp.where(lane16 < 32, last[0], jnp.where(lane16 < 64, last[1], last[2])))
                att[u].append(jnp.concatenate(parts, axis=0) * gate[u][t * C:(t + 1) * C])
        return [jnp.transpose(jnp.concatenate(att[u], axis=0))[:NB] for u in range(2)]

    def g_copy(q):
        return pltpu.make_async_remote_copy(
            src_ref=g_send.at[pl.ds(q * CHUNK, CHUNK)], dst_ref=g_recv.at[pl.ds(q * CHUNK, CHUNK)],
            send_sem=g_ssem.at[q], recv_sem=g_rsem.at[q], device_id={"row": partner}, device_id_type=MESH)

    @pl.loop(0, NCH)
    def _(q):
        for slot, r in enumerate(peers):
            a_wait_recv(slot, q, r)

        @pl.loop(0, CHUNK)
        def _(i):
            p = q * CHUNK + i
            r0, r1 = pair(p)
            gf[pl.ds(s * 48 + p, NB, stride=NB), :] = jnp.where(s == 0, r0, r1)
            g_send[p] = jnp.where(s == 0, r1, r0).astype(BF16)

        g_copy(q).start()

    for q in range(NCH):
        g_copy(q).wait_recv()

    @pl.loop(0, PAIRS, unroll=2)
    def _(p):
        gf[pl.ds((1 - s) * 48 + p, NB, stride=NB), :] = g_recv[p].astype(F32)

    lane_o = lax.rem(lax.broadcasted_iota(jnp.int32, (C, NB), 1), 48)

    @pl.loop(0, NB, unroll=4)
    def _(i):
        gi = gf[pl.ds(pl.multiple_of(i * NB, NB), NB), :].astype(BF16)
        r = dot(wo2[...], gi, 1, 1)
        shifted = jnp.concatenate([jnp.zeros((C, PAIRS), F32), r[C:, :NB - PAIRS]], axis=1)
        upd = jnp.where(lane_o < PAIRS, r[:C], shifted)
        out_ref[i] = (z_ref[i].astype(F32) + upd).astype(BF16)

    for q in range(NCH):
        g_copy(q).wait_send()
        for slot, r in enumerate(peers):
            a_copy(slot, q, r).wait_send()

    @pl.when(jnp.logical_not(is_src))
    def _():
        bias_copy(b_own, u_own, row, b1_ssem, {"row": across}).wait_send()

    for u in range(2):
        for i in range(2):
            @pl.when(sends_right(u))
            def _(u=u, i=i):
                right(u, i).wait_send()

            @pl.when(sends_left(u))
            def _(u=u, i=i):
                left(u, i).wait_send()

            to_partner(u, i).wait_send()


def solution(mesh):
    vm = pl.BlockSpec(memory_space=pltpu.VMEM)
    dma = pltpu.SemaphoreType.DMA

    def body(pair_tile, res_mask, ln_gamma, ln_beta, w_q, w_k, w_v, w_b, w_g, w_o):
        out = pl.pallas_call(
            kernel,
            out_shape=jax.ShapeDtypeStruct((NB, C, NB), BF16),
            in_specs=[vm] * 10,
            out_specs=vm,
            scratch_shapes=[
                pltpu.VMEM((NB * 2 * PAIRS, L), F32),
                pltpu.VMEM((NB, 8, L), F32),
                pltpu.VMEM((2 * PAIRS, NB, L), BF16),
                pltpu.VMEM((PAIRS, NK + 32, L), BF16),
                pltpu.VMEM((3, NB, L), BF16),
                pltpu.VMEM((2, 4, 3, NB, L), BF16),
                pltpu.VMEM((2, 3, NK, L), F32),
                pltpu.VMEM((2, L, 6 * L), BF16),
                pltpu.VMEM((PAIRS, NB, L), BF16),
                pltpu.VMEM((PAIRS, NB, L), BF16),
                pltpu.VMEM((NB * NB, L), F32),
                pltpu.VMEM((L, L), BF16),
                pltpu.VMEM((L, L), BF16),
                pltpu.VMEM((2 * L, L), BF16),
                pltpu.VMEM((L, L), BF16),
                dma((3, NCH)), dma((3, NCH)), dma(()), dma((2, 2, 2)), dma((2, 4)), dma((2, 2)),
                dma((NCH,)), dma((NCH,)),
            ],
            compiler_params=pltpu.CompilerParams(collective_id=0, has_side_effects=True, vmem_limit_bytes=56 * 2**20),
            name="attend",
        )(jnp.transpose(pair_tile, (0, 2, 1)), res_mask, ln_gamma, ln_beta, w_q, w_k, w_v, w_b.T, w_g, w_o)
        return jnp.transpose(out, (0, 2, 1))

    tile_spec = P(("data", "row"), "col", None)
    return jax.shard_map(body, mesh=mesh, in_specs=(tile_spec, P("data"), P(), P(), P(), P(), P(), P(), P(), P()),
                         out_specs=tile_spec, check_vma=False)
```

```python
import math

import jax
import jax.numpy as jnp
from jax import lax
from jax.experimental import pallas as pl
from jax.experimental.pallas import tpu as pltpu
from jax.sharding import PartitionSpec as P

LN_EPS = 1e-5
MASK_FILL = -1e9
LOG2E = math.log2(math.e)
HEADS = 4
HD = 16
C = 64
NB = 96
NK = 384
NQ = 192
PAIRS = 24
CHUNK = 4
NCH = PAIRS // CHUNK
AHEAD = 2
L = 128
MESH = pl.DeviceIdType.MESH
F32 = jnp.float32
BF16 = jnp.bfloat16


def dot(a, b, ca=1, cb=0):
    return lax.dot_general(a, b, (((ca,), (cb,)), ((), ())), preferred_element_type=F32)


def blockdiag2(w):
    z = jnp.zeros_like(w)
    return jnp.concatenate([jnp.concatenate([w, z], 1), jnp.concatenate([z, w], 1)], 0)


def transposed(w):
    return jnp.transpose(w.astype(F32)).astype(BF16)


def down(v, n):
    return jnp.transpose(jnp.broadcast_to(v.reshape(1, n), (L, n)))


def kernel(z_ref, mask_ref, gam_ref, bet_ref, wq_ref, wk_ref, wv_ref, wbt_ref, wg_ref, wo_ref, out_ref,
           t_sc, b_sc, a_nat, a_own, a_all, bias_z, bias_in, bias_f, kbd, vbd, q_sc, gate_sc, p_sc, g_send, g_recv, gf,
           wk2, wv2, wqg2, wo2,
           a_ssem, a_rsem, z_ssem, z_rsem, y_ssem, f_ssem, b_rsem, g_ssem, g_rsem):
    col = lax.axis_index("col")
    row = lax.axis_index("row")
    y, s = row // 2, lax.rem(row, 2)
    partner = y * 2 + (1 - s)
    across = (1 - y) * 2 + s
    cross = (1 - y) * 2 + (1 - s)
    peers = (partner, across, cross)

    barrier = pltpu.get_barrier_semaphore()
    for r in peers:
        pl.semaphore_signal(barrier, inc=1, device_id={"row": r}, device_id_type=MESH)
    for d in range(1, 4):
        pl.semaphore_signal(barrier, inc=1, device_id={"col": lax.rem(col + d, 4)}, device_id_type=MESH)

    gam = down(gam_ref[...], C)[:, :NB]
    bet = down(bet_ref[...], C)[:, :NB]
    wbt = wbt_ref[...]

    @pl.loop(0, NB, unroll=4)
    def _(i):
        z = z_ref[i].astype(F32)
        mean = jnp.sum(z, axis=0, keepdims=True) * (1.0 / C)
        cen = z - mean
        var = jnp.sum(cen * cen, axis=0, keepdims=True) * (1.0 / C)
        a = cen * lax.rsqrt(var + LN_EPS) * gam + bet
        a_nat[i] = a.astype(BF16)
        b_sc[i, :HEADS, :NB] = dot(wbt, a.astype(BF16))

    lane = lax.broadcasted_iota(jnp.int32, (NB, L), 1)
    bh = [b_sc.reshape(NB * 8, L)[pl.ds(h, NB, stride=8), :] for h in range(HEADS)]
    for g in range(3):
        bias_z[col, g] = jnp.where(lane < NB, bh[g], pltpu.roll(bh[3], NB - 32 * g, 1)).astype(BF16)

    pl.semaphore_wait(barrier, 6)

    def z_copy(d):
        return pltpu.make_async_remote_copy(
            src_ref=bias_z.at[col], dst_ref=bias_z.at[col], send_sem=z_ssem.at[d], recv_sem=z_rsem.at[col],
            device_id={"col": lax.rem(col + 1 + d, 4)}, device_id_type=MESH)

    def z_wait(c):
        pltpu.make_async_remote_copy(
            src_ref=bias_z.at[c], dst_ref=bias_z.at[c], send_sem=z_ssem.at[0], recv_sem=z_rsem.at[c],
            device_id={"col": lax.rem(col + 1, 4)}, device_id_type=MESH).wait_recv()

    def bias_copy(src, u, r, ssem, dev):
        return pltpu.make_async_remote_copy(
            src_ref=src, dst_ref=bias_in.at[u, r], send_sem=ssem, recv_sem=b_rsem.at[u, r],
            device_id={"row": dev}, device_id_type=MESH)

    def y_copy(u):
        return bias_copy(bias_z.at[2 * (1 - y) + u], u, row, y_ssem.at[u], across)

    def own_copy(u):
        return bias_copy(bias_z.at[2 * y + u], u, row, f_ssem.at[u, 0], partner)

    def fwd_copy(u):
        return bias_copy(bias_in.at[u, across], u, across, f_ssem.at[u, 1], partner)

    def bias_wait(u, r):
        bias_copy(bias_in.at[u, r], u, r, y_ssem.at[u], partner).wait_recv()

    for d in range(3):
        z_copy(d).start()

    @pl.loop(0, NB, unroll=4)
    def _(i):
        at = jnp.transpose(a_nat[i].astype(F32))
        for half in range(2):
            o = half * 48
            t_sc[pl.ds(pl.multiple_of(i * 48 + half * PAIRS, 8), PAIRS), :] = jnp.concatenate(
                [at[o:o + PAIRS], at[o + PAIRS:o + 2 * PAIRS]], axis=1)

    @pl.loop(0, 2 * PAIRS, unroll=4)
    def _(n):
        a_own[n] = t_sc[pl.ds(n, NB, stride=2 * PAIRS), :].astype(BF16).reshape(3, 32, L)

    def a_desc(slot, q, r, last):
        dst = a_all.at[pl.ds(q * CHUNK, CHUNK), :, 3] if last else a_all.at[pl.ds(q * CHUNK, CHUNK), jnp.minimum(row, 2), 0:3]
        return pltpu.make_async_remote_copy(
            src_ref=a_own.at[pl.ds(lax.rem(r, 2) * PAIRS + q * CHUNK, CHUNK)], dst_ref=dst,
            send_sem=a_ssem.at[slot, q], recv_sem=a_rsem.at[slot, q],
            device_id={"row": r}, device_id_type=MESH)

    def a_start(slot, q):
        @pl.when(row == 3)
        def _():
            a_desc(slot, q, peers[slot], True).start()

        @pl.when(row < 3)
        def _():
            a_desc(slot, q, peers[slot], False).start()

    for q in range(AHEAD):
        for slot in (1, 2, 0):
            a_start(slot, q)

    @pl.when(row == 3)
    def _():
        a_all[:, :, 3] = a_own[pl.ds(s * PAIRS, PAIRS)]

    @pl.when(row < 3)
    def _():
        a_all[:, jnp.minimum(row, 2), 0:3] = a_own[pl.ds(s * PAIRS, PAIRS)]

    wk2[...] = blockdiag2(transposed(wk_ref[...]))
    wv2[...] = blockdiag2(wv_ref[...])
    wqg2[:, :L] = blockdiag2(wq_ref[...])
    wqg2[:, L:] = blockdiag2(wg_ref[...])
    wo2[...] = blockdiag2(wo_ref[...])
    for par in range(2):
        for t in range(2):
            kbd[par, t] = jnp.zeros((C, HEADS * NK), BF16)

    for u in range(2):
        @pl.when(2 * (1 - y) + u != col)
        def _(u=u):
            z_wait(2 * (1 - y) + u)
        y_copy(u).start()
    for q in range(AHEAD, NCH):
        for slot in (1, 2, 0):
            a_start(slot, q)
    for u in range(2):
        @pl.when(2 * y + u != col)
        def _(u=u):
            z_wait(2 * y + u)
        own_copy(u).start()
        bias_in[u, row] = bias_z[2 * y + u]
    for u in range(2):
        bias_wait(u, across)
        fwd_copy(u).start()
    for u in range(2):
        for r in (partner, cross):
            bias_wait(u, r)

    fill = down(jnp.where(mask_ref[...] > 0, 0.0, MASK_FILL).astype(F32), NK)
    for u in range(2):
        for g in range(3):
            parts = []
            for t in range(3):
                parts.append(bias_in[u, t, g].astype(F32) + fill[t * NB:(t + 1) * NB])
                parts.append(bias_in[u, 3, g, t * 32:(t + 1) * 32].astype(F32) + fill[3 * NB + t * 32:3 * NB + (t + 1) * 32])
            bt = jnp.transpose(jnp.concatenate(parts, axis=0)) * LOG2E
            bias_f[g, u * NB:(u + 1) * NB, :] = bt[:NB]
            bias_f[3, u * NB + g * 32:u * NB + (g + 1) * 32, :] = bt[NB:]

    hid = lax.broadcasted_iota(jnp.int32, (NK, C), 1) // HD
    hid_q = lax.broadcasted_iota(jnp.int32, (NQ, C), 1) // HD

    def project(p, par):
        x = a_all[p].reshape(NK, L)
        x_lo = a_all[p, 0:2, 0:3].reshape(NQ, L)
        x_hi = jnp.concatenate([a_all[p, 2, 0:3].reshape(NB, L), a_all[p, :, 3].reshape(NB, L)], axis=0)
        qg = dot(jnp.where(y == 0, x_lo, x_hi), wqg2[...])
        v2 = dot(x, wv2[...]).astype(BF16)
        kt = dot(wk2[...], x, 1, 1).astype(BF16)
        gate_sc[par] = jax.nn.sigmoid(qg[:, L:])
        for t in range(2):
            q_sc[par, t] = (qg[:, t * C:(t + 1) * C] * (1.0 / math.sqrt(HD))).astype(BF16)
            v_t = v2[:, t * C:(t + 1) * C]
            for h in range(HEADS):
                kbd[par, t, h * HD:(h + 1) * HD, h * NK:(h + 1) * NK] = kt[t * C + h * HD:t * C + (h + 1) * HD, :]
                vbd[par, t, h * NK:(h + 1) * NK, :] = jnp.where(hid == h, v_t, jnp.zeros_like(v_t))

    def attend(p, par):
        gated = []
        for t in range(2):
            inv = []
            for hp in range(2):
                logits = dot(q_sc[par, t], kbd[par, t, :, hp * 2 * NK:(hp + 1) * 2 * NK])
                for hh in range(2):
                    h = hp * 2 + hh
                    lt = logits[:, hh * NK:(hh + 1) * NK] * LOG2E + bias_f[h]
                    e = jnp.exp2(lt - jnp.max(lt, axis=1, keepdims=True))
                    inv.append(1.0 / jnp.sum(e, axis=1, keepdims=True))
                    p_sc[t, :, h * NK:(h + 1) * NK] = e.astype(BF16)
            o = dot(p_sc[t], vbd[par, t])
            scale = jnp.where(hid_q == 0, inv[0], jnp.where(hid_q == 1, inv[1], jnp.where(hid_q == 2, inv[2], inv[3])))
            gated.append(gate_sc[par, :, t * C:(t + 1) * C] * (o * scale))
        res = jnp.concatenate(gated, axis=1)
        gf[pl.ds(s * PAIRS + p, NB, stride=2 * PAIRS), :] = jnp.where(s == 0, res[:NB], res[NB:])
        g_send[p] = jnp.where(s == 0, res[NB:], res[:NB]).astype(BF16)

    def g_copy(q):
        return pltpu.make_async_remote_copy(
            src_ref=g_send.at[pl.ds(q * CHUNK, CHUNK)], dst_ref=g_recv.at[pl.ds(q * CHUNK, CHUNK)],
            send_sem=g_ssem.at[q], recv_sem=g_rsem.at[q], device_id={"row": partner}, device_id_type=MESH)

    def a_wait(q):
        for slot in range(3):
            a_desc(slot, q, peers[slot], False).wait_recv()

    a_wait(0)
    project(0, 0)

    @pl.loop(0, NCH)
    def _(q):
        @pl.loop(0, CHUNK // 2)
        def _(i):
            p = q * CHUNK + 2 * i

            @pl.when(jnp.logical_and(i == CHUNK // 2 - 1, q < NCH - 1))
            def _():
                a_wait(q + 1)

            project(p + 1, 1)
            attend(p, 0)
            project(jnp.minimum(p + 2, PAIRS - 1), 0)
            attend(p + 1, 1)

        g_copy(q).start()

    for q in range(NCH):
        g_copy(q).wait_recv()

    @pl.loop(0, PAIRS, unroll=4)
    def _(p):
        gf[pl.ds((1 - s) * PAIRS + p, NB, stride=2 * PAIRS), :] = g_recv[p].astype(F32)

    @pl.loop(0, NB // 4, unroll=2)
    def _(i4):
        r4 = dot(gf[pl.ds(pl.multiple_of(i4 * 192, 8), 192), :].astype(BF16), wo2[...])
        for k in range(4):
            r = r4[k * 48:(k + 1) * 48]
            rr = pltpu.roll(r, C, 1)
            jc = jnp.concatenate([r[:PAIRS], rr[:PAIRS], r[PAIRS:], rr[PAIRS:]], axis=0)
            i = i4 * 4 + k
            out_ref[i] = (z_ref[i].astype(F32) + jnp.transpose(jc)[:C]).astype(BF16)

    for q in range(NCH):
        g_copy(q).wait_send()
        for slot in range(3):
            a_desc(slot, q, peers[slot], False).wait_send()
    for d in range(3):
        z_copy(d).wait_send()
    for u in range(2):
        y_copy(u).wait_send()
        own_copy(u).wait_send()
        fwd_copy(u).wait_send()


def solution(mesh):
    vm = pl.BlockSpec(memory_space=pltpu.VMEM)
    dma = pltpu.SemaphoreType.DMA

    def body(pair_tile, res_mask, ln_gamma, ln_beta, w_q, w_k, w_v, w_b, w_g, w_o):
        out = pl.pallas_call(
            kernel,
            out_shape=jax.ShapeDtypeStruct((NB, C, NB), BF16),
            in_specs=[vm] * 10,
            out_specs=vm,
            scratch_shapes=[
                pltpu.VMEM((NB * 2 * PAIRS, L), F32),
                pltpu.VMEM((NB, 8, L), F32),
                pltpu.VMEM((NB, C, NB), BF16),
                pltpu.VMEM((2 * PAIRS, 3, 32, L), BF16),
                pltpu.VMEM((PAIRS, 3, 4, 32, L), BF16),
                pltpu.VMEM((4, 3, NB, L), BF16),
                pltpu.VMEM((2, 4, 3, NB, L), BF16),
                pltpu.VMEM((HEADS, NQ, NK), F32),
                pltpu.VMEM((2, 2, C, HEADS * NK), BF16),
                pltpu.VMEM((2, 2, HEADS * NK, C), BF16),
                pltpu.VMEM((2, 2, NQ, C), BF16),
                pltpu.VMEM((2, NQ, L), F32),
                pltpu.VMEM((2, NQ, HEADS * NK), BF16),
                pltpu.VMEM((PAIRS, NB, L), BF16),
                pltpu.VMEM((PAIRS, NB, L), BF16),
                pltpu.VMEM((NB * 2 * PAIRS, L), F32),
                pltpu.VMEM((L, L), BF16),
                pltpu.VMEM((L, L), BF16),
                pltpu.VMEM((L, 2 * L), BF16),
                pltpu.VMEM((L, L), BF16),
                dma((3, NCH)), dma((3, NCH)), dma((3,)), dma((4,)), dma((2,)), dma((2, 2)), dma((2, 4)),
                dma((NCH,)), dma((NCH,)),
            ],
            compiler_params=pltpu.CompilerParams(collective_id=0, has_side_effects=True, vmem_limit_bytes=56 * 2**20),
            name="attend",
        )(jnp.transpose(pair_tile, (0, 2, 1)), res_mask, ln_gamma, ln_beta, w_q, w_k, w_v, w_b.T, w_g, w_o)
        return jnp.transpose(out, (0, 2, 1))

    tile_spec = P(("data", "row"), "col", None)
    return jax.shard_map(body, mesh=mesh, in_specs=(tile_spec, P("data"), P(), P(), P(), P(), P(), P(), P(), P()),
                         out_specs=tile_spec, check_vma=False)
```

```python
import math

import jax
import jax.numpy as jnp
from jax import lax
from jax.experimental import pallas as pl
from jax.experimental.pallas import tpu as pltpu
from jax.sharding import PartitionSpec as P

LN_EPS = 1e-5
MASK_FILL = -1e9
LOG2E = math.log2(math.e)
HEADS = 4
HD = 16
C = 64
NB = 96
NK = 384
NQ = 192
PAIRS = 24
CHUNK = 4
NCH = PAIRS // CHUNK
AHEAD = 1
L = 128
MESH = pl.DeviceIdType.MESH
F32 = jnp.float32
BF16 = jnp.bfloat16


def dot(a, b, ca=1, cb=0):
    return lax.dot_general(a, b, (((ca,), (cb,)), ((), ())), preferred_element_type=F32)


def blockdiag2(w):
    z = jnp.zeros_like(w)
    return jnp.concatenate([jnp.concatenate([w, z], 1), jnp.concatenate([z, w], 1)], 0)


def transposed(w):
    return jnp.transpose(w.astype(F32)).astype(BF16)


def down(v, n):
    return jnp.transpose(jnp.broadcast_to(v.reshape(1, n), (L, n)))


def kernel(z_ref, mask_ref, gam_ref, bet_ref, wq_ref, wk_ref, wv_ref, wbt_ref, wg_ref, wo_ref, out_ref,
           t_sc, b_sc, a_nat, a_own, a_all, bias_z, bias_in, bias_f, kbd, vbd, q_sc, gate_sc, p_sc, g_send, g_recv, gf,
           wk2, wv2, wqg2, wo4,
           a_ssem, a_rsem, z_ssem, z_rsem, y_ssem, f_ssem, b_rsem, g_ssem, g_rsem):
    col = lax.axis_index("col")
    row = lax.axis_index("row")
    y, s = row // 2, lax.rem(row, 2)
    partner = y * 2 + (1 - s)
    across = (1 - y) * 2 + s
    cross = (1 - y) * 2 + (1 - s)
    peers = (partner, across, cross)

    barrier = pltpu.get_barrier_semaphore()
    for r in peers:
        pl.semaphore_signal(barrier, inc=1, device_id={"row": r}, device_id_type=MESH)
    for d in range(1, 4):
        pl.semaphore_signal(barrier, inc=1, device_id={"col": lax.rem(col + d, 4)}, device_id_type=MESH)

    gam = down(gam_ref[...], C)[:, :NB]
    bet = down(bet_ref[...], C)[:, :NB]
    wbt = wbt_ref[...]

    @pl.loop(0, NB, unroll=4)
    def _(i):
        z = z_ref[i].astype(F32)
        mean = jnp.sum(z, axis=0, keepdims=True) * (1.0 / C)
        cen = z - mean
        var = jnp.sum(cen * cen, axis=0, keepdims=True) * (1.0 / C)
        a = cen * lax.rsqrt(var + LN_EPS) * gam + bet
        a_nat[i] = a.astype(BF16)
        b_sc[i, :HEADS, :NB] = dot(wbt, a.astype(BF16))

    lane = lax.broadcasted_iota(jnp.int32, (NB, L), 1)
    bh = [b_sc.reshape(NB * 8, L)[pl.ds(h, NB, stride=8), :] for h in range(HEADS)]
    for g in range(3):
        bias_z[col, g] = jnp.where(lane < NB, bh[g], pltpu.roll(bh[3], NB - 32 * g, 1)).astype(BF16)

    pl.semaphore_wait(barrier, 6)

    def z_copy(d):
        return pltpu.make_async_remote_copy(
            src_ref=bias_z.at[col], dst_ref=bias_z.at[col], send_sem=z_ssem.at[d], recv_sem=z_rsem.at[col],
            device_id={"col": lax.rem(col + 1 + d, 4)}, device_id_type=MESH)

    def z_wait(c):
        pltpu.make_async_remote_copy(
            src_ref=bias_z.at[c], dst_ref=bias_z.at[c], send_sem=z_ssem.at[0], recv_sem=z_rsem.at[c],
            device_id={"col": lax.rem(col + 1, 4)}, device_id_type=MESH).wait_recv()

    def bias_copy(src, u, r, ssem, dev):
        return pltpu.make_async_remote_copy(
            src_ref=src, dst_ref=bias_in.at[u, r], send_sem=ssem, recv_sem=b_rsem.at[u, r],
            device_id={"row": dev}, device_id_type=MESH)

    def y_copy(u):
        return bias_copy(bias_z.at[2 * (1 - y) + u], u, row, y_ssem.at[u], across)

    def own_copy(u):
        return bias_copy(bias_z.at[2 * y + u], u, row, f_ssem.at[u, 0], partner)

    def fwd_copy(u):
        return bias_copy(bias_in.at[u, across], u, across, f_ssem.at[u, 1], partner)

    def bias_wait(u, r):
        bias_copy(bias_in.at[u, r], u, r, y_ssem.at[u], partner).wait_recv()

    for d in range(3):
        z_copy(d).start()

    lane_t = lax.broadcasted_iota(jnp.int32, (PAIRS, L), 1)

    @pl.loop(0, NB // 2, unroll=2)
    def _(i2):
        at = jnp.transpose(jnp.concatenate([a_nat[2 * i2], a_nat[2 * i2 + 1]], axis=0).astype(F32))
        for half in range(2):
            o = half * 48
            lo, hi = at[o:o + PAIRS], at[o + PAIRS:o + 2 * PAIRS]
            base = pl.multiple_of(i2 * 96 + half * PAIRS, 8)
            t_sc[pl.ds(base, PAIRS), :] = jnp.where(lane_t < C, lo, pltpu.roll(hi, C, 1))
            t_sc[pl.ds(base + 48, PAIRS), :] = jnp.where(lane_t < C, pltpu.roll(lo, C, 1), hi)

    @pl.loop(0, 2 * PAIRS, unroll=4)
    def _(n):
        a_own[n] = t_sc[pl.ds(n, NB, stride=2 * PAIRS), :].astype(BF16).reshape(3, 32, L)

    def a_desc(slot, q, r, last):
        dst = a_all.at[pl.ds(q * CHUNK, CHUNK), :, 3] if last else a_all.at[pl.ds(q * CHUNK, CHUNK), jnp.minimum(row, 2), 0:3]
        return pltpu.make_async_remote_copy(
            src_ref=a_own.at[pl.ds(lax.rem(r, 2) * PAIRS + q * CHUNK, CHUNK)], dst_ref=dst,
            send_sem=a_ssem.at[slot, q], recv_sem=a_rsem.at[slot, q],
            device_id={"row": r}, device_id_type=MESH)

    def a_start(slot, q):
        @pl.when(row == 3)
        def _():
            a_desc(slot, q, peers[slot], True).start()

        @pl.when(row < 3)
        def _():
            a_desc(slot, q, peers[slot], False).start()

    for q in range(AHEAD):
        for slot in (1, 2, 0):
            a_start(slot, q)

    @pl.when(row == 3)
    def _():
        a_all[:, :, 3] = a_own[pl.ds(s * PAIRS, PAIRS)]

    @pl.when(row < 3)
    def _():
        a_all[:, jnp.minimum(row, 2), 0:3] = a_own[pl.ds(s * PAIRS, PAIRS)]

    wk2[...] = blockdiag2(transposed(wk_ref[...]))
    wv2[...] = blockdiag2(wv_ref[...])
    wqg2[:, :L] = blockdiag2(wq_ref[...])
    wqg2[:, L:] = blockdiag2(wg_ref[...])
    wo = wo_ref[...]
    wo4[:, :L] = blockdiag2(wo)
    wo4[:, L:] = jnp.concatenate([jnp.concatenate([jnp.zeros_like(wo), wo], 1), jnp.concatenate([wo, jnp.zeros_like(wo)], 1)], 0)
    for par in range(2):
        for t in range(2):
            kbd[par, t] = jnp.zeros((C, HEADS * NK), BF16)

    for u in range(2):
        @pl.when(2 * (1 - y) + u != col)
        def _(u=u):
            z_wait(2 * (1 - y) + u)
        y_copy(u).start()
    for q in range(AHEAD, NCH):
        for slot in (1, 2, 0):
            a_start(slot, q)
    for u in range(2):
        @pl.when(2 * y + u != col)
        def _(u=u):
            z_wait(2 * y + u)
        own_copy(u).start()
        bias_in[u, row] = bias_z[2 * y + u]
    for u in range(2):
        bias_wait(u, across)
        fwd_copy(u).start()
    for u in range(2):
        for r in (partner, cross):
            bias_wait(u, r)

    fill = down(jnp.where(mask_ref[...] > 0, 0.0, MASK_FILL).astype(F32), NK)
    for u in range(2):
        for g in range(3):
            parts = []
            for t in range(3):
                parts.append(bias_in[u, t, g].astype(F32) + fill[t * NB:(t + 1) * NB])
                parts.append(bias_in[u, 3, g, t * 32:(t + 1) * 32].astype(F32) + fill[3 * NB + t * 32:3 * NB + (t + 1) * 32])
            bt = jnp.transpose(jnp.concatenate(parts, axis=0)) * LOG2E
            bias_f[g, u * NB:(u + 1) * NB, :] = bt[:NB]
            bias_f[3, u * NB + g * 32:u * NB + (g + 1) * 32, :] = bt[NB:]

    hid = lax.broadcasted_iota(jnp.int32, (NK, C), 1) // HD
    hid_q = lax.broadcasted_iota(jnp.int32, (NQ, C), 1) // HD

    def project(p, par):
        x = a_all[p].reshape(NK, L)
        x_lo = a_all[p, 0:2, 0:3].reshape(NQ, L)
        x_hi = jnp.concatenate([a_all[p, 2, 0:3].reshape(NB, L), a_all[p, :, 3].reshape(NB, L)], axis=0)
        qg = dot(jnp.where(y == 0, x_lo, x_hi), wqg2[...])
        v2 = dot(x, wv2[...]).astype(BF16)
        kt = dot(wk2[...], x, 1, 1).astype(BF16)
        gate_sc[par] = jax.nn.sigmoid(qg[:, L:])
        for t in range(2):
            q_sc[par, t] = (qg[:, t * C:(t + 1) * C] * (1.0 / math.sqrt(HD))).astype(BF16)
            v_t = v2[:, t * C:(t + 1) * C]
            for h in range(HEADS):
                kbd[par, t, h * HD:(h + 1) * HD, h * NK:(h + 1) * NK] = kt[t * C + h * HD:t * C + (h + 1) * HD, :]
                vbd[par, t, h * NK:(h + 1) * NK, :] = jnp.where(hid == h, v_t, jnp.zeros_like(v_t))

    def attend(p, par):
        gated = []
        for t in range(2):
            inv = []
            for hp in range(2):
                logits = dot(q_sc[par, t], kbd[par, t, :, hp * 2 * NK:(hp + 1) * 2 * NK])
                for hh in range(2):
                    h = hp * 2 + hh
                    lt = logits[:, hh * NK:(hh + 1) * NK] * LOG2E + bias_f[h]
                    e = jnp.exp2(lt - jnp.max(lt, axis=1, keepdims=True))
                    inv.append(1.0 / jnp.sum(e, axis=1, keepdims=True))
                    p_sc[t, :, h * NK:(h + 1) * NK] = e.astype(BF16)
            o = dot(p_sc[t], vbd[par, t])
            scale = jnp.where(hid_q == 0, inv[0], jnp.where(hid_q == 1, inv[1], jnp.where(hid_q == 2, inv[2], inv[3])))
            gated.append(gate_sc[par, :, t * C:(t + 1) * C] * (o * scale))
        res = jnp.concatenate(gated, axis=1)
        gf[pl.ds(s * PAIRS + p, NB, stride=2 * PAIRS), :] = jnp.where(s == 0, res[:NB], res[NB:])
        g_send[p] = jnp.where(s == 0, res[NB:], res[:NB]).astype(BF16)

    def g_copy(q):
        return pltpu.make_async_remote_copy(
            src_ref=g_send.at[pl.ds(q * CHUNK, CHUNK)], dst_ref=g_recv.at[pl.ds(q * CHUNK, CHUNK)],
            send_sem=g_ssem.at[q], recv_sem=g_rsem.at[q], device_id={"row": partner}, device_id_type=MESH)

    def a_wait(q):
        for slot in range(3):
            a_desc(slot, q, peers[slot], False).wait_recv()

    a_wait(0)
    project(0, 0)

    @pl.loop(0, NCH)
    def _(q):
        @pl.loop(0, CHUNK // 2)
        def _(i):
            p = q * CHUNK + 2 * i

            @pl.when(jnp.logical_and(i == CHUNK // 2 - 1, q < NCH - 1))
            def _():
                a_wait(q + 1)

            project(p + 1, 1)
            attend(p, 0)
            project(jnp.minimum(p + 2, PAIRS - 1), 0)
            attend(p + 1, 1)

        g_copy(q).start()

    for q in range(NCH):
        g_copy(q).wait_recv()

    @pl.loop(0, PAIRS, unroll=4)
    def _(p):
        gf[pl.ds((1 - s) * PAIRS + p, NB, stride=2 * PAIRS), :] = g_recv[p].astype(F32)

    lane_o = lax.broadcasted_iota(jnp.int32, (2 * PAIRS, L), 1)

    @pl.loop(0, NB // 4, unroll=2)
    def _(i4):
        r4 = dot(gf[pl.ds(pl.multiple_of(i4 * 192, 8), 192), :].astype(BF16), wo4[...])
        for k in range(2):
            ra, rb = r4[k * 96:k * 96 + 48], r4[k * 96 + 48:(k + 1) * 96]
            c0 = jnp.where(lane_o < C, ra[:, :L], rb[:, L:])
            c1 = jnp.where(lane_o < C, ra[:, L:], rb[:, :L])
            both = jnp.transpose(jnp.concatenate([c0[:PAIRS], c1[:PAIRS], c0[PAIRS:], c1[PAIRS:]], axis=0))
            i = i4 * 4 + 2 * k
            out_ref[i] = (z_ref[i].astype(F32) + both[:C]).astype(BF16)
            out_ref[i + 1] = (z_ref[i + 1].astype(F32) + both[C:]).astype(BF16)

    for q in range(NCH):
        g_copy(q).wait_send()
        for slot in range(3):
            a_desc(slot, q, peers[slot], False).wait_send()
    for d in range(3):
        z_copy(d).wait_send()
    for u in range(2):
        y_copy(u).wait_send()
        own_copy(u).wait_send()
        fwd_copy(u).wait_send()


def solution(mesh):
    vm = pl.BlockSpec(memory_space=pltpu.VMEM)
    dma = pltpu.SemaphoreType.DMA

    def body(pair_tile, res_mask, ln_gamma, ln_beta, w_q, w_k, w_v, w_b, w_g, w_o):
        out = pl.pallas_call(
            kernel,
            out_shape=jax.ShapeDtypeStruct((NB, C, NB), BF16),
            in_specs=[vm] * 10,
            out_specs=vm,
            scratch_shapes=[
                pltpu.VMEM((NB * 2 * PAIRS, L), F32),
                pltpu.VMEM((NB, 8, L), F32),
                pltpu.VMEM((NB, C, NB), BF16),
                pltpu.VMEM((2 * PAIRS, 3, 32, L), BF16),
                pltpu.VMEM((PAIRS, 3, 4, 32, L), BF16),
                pltpu.VMEM((4, 3, NB, L), BF16),
                pltpu.VMEM((2, 4, 3, NB, L), BF16),
                pltpu.VMEM((HEADS, NQ, NK), F32),
                pltpu.VMEM((2, 2, C, HEADS * NK), BF16),
                pltpu.VMEM((2, 2, HEADS * NK, C), BF16),
                pltpu.VMEM((2, 2, NQ, C), BF16),
                pltpu.VMEM((2, NQ, L), F32),
                pltpu.VMEM((2, NQ, HEADS * NK), BF16),
                pltpu.VMEM((PAIRS, NB, L), BF16),
                pltpu.VMEM((PAIRS, NB, L), BF16),
                pltpu.VMEM((NB * 2 * PAIRS, L), F32),
                pltpu.VMEM((L, L), BF16),
                pltpu.VMEM((L, L), BF16),
                pltpu.VMEM((L, 2 * L), BF16),
                pltpu.VMEM((L, 2 * L), BF16),
                dma((3, NCH)), dma((3, NCH)), dma((3,)), dma((4,)), dma((2,)), dma((2, 2)), dma((2, 4)),
                dma((NCH,)), dma((NCH,)),
            ],
            compiler_params=pltpu.CompilerParams(collective_id=0, has_side_effects=True, vmem_limit_bytes=56 * 2**20),
            name="attend",
        )(jnp.transpose(pair_tile, (0, 2, 1)), res_mask, ln_gamma, ln_beta, w_q, w_k, w_v, w_b.T, w_g, w_o)
        return jnp.transpose(out, (0, 2, 1))

    tile_spec = P(("data", "row"), "col", None)
    return jax.shard_map(body, mesh=mesh, in_specs=(tile_spec, P("data"), P(), P(), P(), P(), P(), P(), P(), P()),
                         out_specs=tile_spec, check_vma=False)
```

```python
import math

import jax
import jax.numpy as jnp
from jax import lax
from jax.experimental import pallas as pl
from jax.experimental.pallas import tpu as pltpu
from jax.sharding import PartitionSpec as P

LN_EPS = 1e-5
MASK_FILL = -1e9
LOG2E = math.log2(math.e)
HEADS = 4
HD = 16
C = 64
NB = 96
NK = 384
NQ = 192
PAIRS = 24
CHUNK = 2
NCH = PAIRS // CHUNK
AHEAD = 1
L = 128
MESH = pl.DeviceIdType.MESH
F32 = jnp.float32
BF16 = jnp.bfloat16


def dot(a, b, ca=1, cb=0):
    return lax.dot_general(a, b, (((ca,), (cb,)), ((), ())), preferred_element_type=F32)


def blockdiag2(w):
    z = jnp.zeros_like(w)
    return jnp.concatenate([jnp.concatenate([w, z], 1), jnp.concatenate([z, w], 1)], 0)


def transposed(w):
    return jnp.transpose(w.astype(F32)).astype(BF16)


def down(v, n):
    return jnp.transpose(jnp.broadcast_to(v.reshape(1, n), (L, n)))


def kernel(z_ref, mask_ref, gam_ref, bet_ref, wq_ref, wk_ref, wv_ref, wbt_ref, wg_ref, wo_ref, out_ref,
           t_sc, b_sc, a_nat, a_own, a_all, bias_z, bias_in, bias_f, kbd, vbd, q_sc, gate_sc, p_sc, g_send, g_recv, gf,
           wk2, wv2, wqg2, wo4,
           a_ssem, a_rsem, z_ssem, z_rsem, y_ssem, f_ssem, b_rsem, g_ssem, g_rsem):
    col = lax.axis_index("col")
    row = lax.axis_index("row")
    y, s = row // 2, lax.rem(row, 2)
    partner = y * 2 + (1 - s)
    across = (1 - y) * 2 + s
    cross = (1 - y) * 2 + (1 - s)
    peers = (partner, across, cross)

    barrier = pltpu.get_barrier_semaphore()
    for r in peers:
        pl.semaphore_signal(barrier, inc=1, device_id={"row": r}, device_id_type=MESH)
    for d in range(1, 4):
        pl.semaphore_signal(barrier, inc=1, device_id={"col": lax.rem(col + d, 4)}, device_id_type=MESH)

    gam = down(gam_ref[...], C)[:, :NB]
    bet = down(bet_ref[...], C)[:, :NB]
    wbt = wbt_ref[...]

    @pl.loop(0, NB, unroll=4)
    def _(i):
        z = z_ref[i].astype(F32)
        mean = jnp.sum(z, axis=0, keepdims=True) * (1.0 / C)
        cen = z - mean
        var = jnp.sum(cen * cen, axis=0, keepdims=True) * (1.0 / C)
        a = cen * lax.rsqrt(var + LN_EPS) * gam + bet
        a_nat[i] = a.astype(BF16)
        b_sc[i, :HEADS, :NB] = dot(wbt, a.astype(BF16))

    lane = lax.broadcasted_iota(jnp.int32, (NB, L), 1)
    bh = [b_sc.reshape(NB * 8, L)[pl.ds(h, NB, stride=8), :] for h in range(HEADS)]
    for g in range(3):
        bias_z[col, g] = jnp.where(lane < NB, bh[g], pltpu.roll(bh[3], NB - 32 * g, 1)).astype(BF16)

    pl.semaphore_wait(barrier, 6)

    def z_copy(d):
        return pltpu.make_async_remote_copy(
            src_ref=bias_z.at[col], dst_ref=bias_z.at[col], send_sem=z_ssem.at[d], recv_sem=z_rsem.at[col],
            device_id={"col": lax.rem(col + 1 + d, 4)}, device_id_type=MESH)

    def z_wait(c):
        pltpu.make_async_remote_copy(
            src_ref=bias_z.at[c], dst_ref=bias_z.at[c], send_sem=z_ssem.at[0], recv_sem=z_rsem.at[c],
            device_id={"col": lax.rem(col + 1, 4)}, device_id_type=MESH).wait_recv()

    def bias_copy(src, u, r, ssem, dev):
        return pltpu.make_async_remote_copy(
            src_ref=src, dst_ref=bias_in.at[u, r], send_sem=ssem, recv_sem=b_rsem.at[u, r],
            device_id={"row": dev}, device_id_type=MESH)

    def y_copy(u):
        return bias_copy(bias_z.at[2 * (1 - y) + u], u, row, y_ssem.at[u], across)

    def own_copy(u):
        return bias_copy(bias_z.at[2 * y + u], u, row, f_ssem.at[u, 0], partner)

    def fwd_copy(u):
        return bias_copy(bias_in.at[u, across], u, across, f_ssem.at[u, 1], partner)

    def bias_wait(u, r):
        bias_copy(bias_in.at[u, r], u, r, y_ssem.at[u], partner).wait_recv()

    for d in range(3):
        z_copy(d).start()

    lane_t = lax.broadcasted_iota(jnp.int32, (PAIRS, L), 1)

    @pl.loop(0, NB // 2, unroll=2)
    def _(i2):
        at = jnp.transpose(jnp.concatenate([a_nat[2 * i2], a_nat[2 * i2 + 1]], axis=0).astype(F32))
        for half in range(2):
            o = half * 48
            lo, hi = at[o:o + PAIRS], at[o + PAIRS:o + 2 * PAIRS]
            base = pl.multiple_of(i2 * 96 + half * PAIRS, 8)
            t_sc[pl.ds(base, PAIRS), :] = jnp.where(lane_t < C, lo, pltpu.roll(hi, C, 1))
            t_sc[pl.ds(base + 48, PAIRS), :] = jnp.where(lane_t < C, pltpu.roll(lo, C, 1), hi)

    @pl.loop(0, 2 * PAIRS, unroll=4)
    def _(n):
        a_own[n] = t_sc[pl.ds(n, NB, stride=2 * PAIRS), :].astype(BF16).reshape(3, 32, L)

    def a_desc(slot, q, r, last):
        dst = a_all.at[pl.ds(q * CHUNK, CHUNK), :, 3] if last else a_all.at[pl.ds(q * CHUNK, CHUNK), jnp.minimum(row, 2), 0:3]
        return pltpu.make_async_remote_copy(
            src_ref=a_own.at[pl.ds(lax.rem(r, 2) * PAIRS + q * CHUNK, CHUNK)], dst_ref=dst,
            send_sem=a_ssem.at[slot, q], recv_sem=a_rsem.at[slot, q],
            device_id={"row": r}, device_id_type=MESH)

    def a_start(slot, q):
        @pl.when(row == 3)
        def _():
            a_desc(slot, q, peers[slot], True).start()

        @pl.when(row < 3)
        def _():
            a_desc(slot, q, peers[slot], False).start()

    for q in range(AHEAD):
        for slot in (1, 2, 0):
            a_start(slot, q)

    @pl.when(row == 3)
    def _():
        a_all[:, :, 3] = a_own[pl.ds(s * PAIRS, PAIRS)]

    @pl.when(row < 3)
    def _():
        a_all[:, jnp.minimum(row, 2), 0:3] = a_own[pl.ds(s * PAIRS, PAIRS)]

    wk2[...] = blockdiag2(transposed(wk_ref[...]))
    wv2[...] = blockdiag2(wv_ref[...])
    wqg2[:, :L] = blockdiag2(wq_ref[...])
    wqg2[:, L:] = blockdiag2(wg_ref[...])
    wo = wo_ref[...]
    wo4[:, :L] = blockdiag2(wo)
    wo4[:, L:] = jnp.concatenate([jnp.concatenate([jnp.zeros_like(wo), wo], 1), jnp.concatenate([wo, jnp.zeros_like(wo)], 1)], 0)
    for par in range(2):
        for t in range(2):
            kbd[par, t] = jnp.zeros((C, HEADS * NK), BF16)

    for u in range(2):
        @pl.when(2 * (1 - y) + u != col)
        def _(u=u):
            z_wait(2 * (1 - y) + u)
        y_copy(u).start()
    for q in range(AHEAD, NCH):
        for slot in (1, 2, 0):
            a_start(slot, q)
    for u in range(2):
        @pl.when(2 * y + u != col)
        def _(u=u):
            z_wait(2 * y + u)
        own_copy(u).start()
        bias_in[u, row] = bias_z[2 * y + u]
    for u in range(2):
        bias_wait(u, across)
        fwd_copy(u).start()
    for u in range(2):
        for r in (partner, cross):
            bias_wait(u, r)

    fill = down(jnp.where(mask_ref[...] > 0, 0.0, MASK_FILL).astype(F32), NK)
    for u in range(2):
        for g in range(3):
            parts = []
            for t in range(3):
                parts.append(bias_in[u, t, g].astype(F32) + fill[t * NB:(t + 1) * NB])
                parts.append(bias_in[u, 3, g, t * 32:(t + 1) * 32].astype(F32) + fill[3 * NB + t * 32:3 * NB + (t + 1) * 32])
            bt = jnp.transpose(jnp.concatenate(parts, axis=0)) * LOG2E
            bias_f[g, u * NB:(u + 1) * NB, :] = bt[:NB]
            bias_f[3, u * NB + g * 32:u * NB + (g + 1) * 32, :] = bt[NB:]

    hid = lax.rem(lax.broadcasted_iota(jnp.int32, (NK, L), 1), C) // HD
    lane_q = lax.broadcasted_iota(jnp.int32, (NQ, L), 1)
    hid_q = lax.rem(lane_q, C) // HD

    def project(p, par):
        x = a_all[p].reshape(NK, L)
        x_lo = a_all[p, 0:2, 0:3].reshape(NQ, L)
        x_hi = jnp.concatenate([a_all[p, 2, 0:3].reshape(NB, L), a_all[p, :, 3].reshape(NB, L)], axis=0)
        qg = dot(jnp.where(y == 0, x_lo, x_hi), wqg2[...])
        v2 = dot(x, wv2[...]).astype(BF16)
        kt = dot(wk2[...], x, 1, 1).astype(BF16)
        gate_sc[par] = jax.nn.sigmoid(qg[:, L:])
        q2 = (qg[:, :L] * (1.0 / math.sqrt(HD))).astype(BF16)
        for h in range(HEADS):
            vbd[par, h * NK:(h + 1) * NK, :] = jnp.where(hid == h, v2, jnp.zeros_like(v2))
        for t in range(2):
            q_sc[par, t, :, :C] = q2[:, t * C:(t + 1) * C]
            for h in range(HEADS):
                kbd[par, t, h * HD:(h + 1) * HD, h * NK:(h + 1) * NK] = kt[t * C + h * HD:t * C + (h + 1) * HD, :]

    def softmax(t, logits):
        sums = []
        for h in range(HEADS):
            lt = logits[:, h * NK:(h + 1) * NK] * LOG2E + bias_f[h]
            e = jnp.exp2(lt - jnp.max(lt, axis=1, keepdims=True))
            sums.append(jnp.sum(e, axis=1, keepdims=True))
            p_sc[t, :, h * NK:(h + 1) * NK] = e.astype(BF16)
        return sums

    def attend(p, par):
        logits = [dot(q_sc[par, t, :, :C], kbd[par, t]) for t in range(2)]
        sums = [softmax(t, logits[t]) for t in range(2)]
        o = []
        for t in range(2):
            l = sums[t]
            div = jnp.where(hid_q == 0, l[0], jnp.where(hid_q == 1, l[1], jnp.where(hid_q == 2, l[2], l[3])))
            o.append(dot(p_sc[t], vbd[par]) / div)
        res = gate_sc[par] * jnp.where(lane_q < C, o[0], o[1])
        gf[pl.ds(s * PAIRS + p, NB, stride=2 * PAIRS), :] = jnp.where(s == 0, res[:NB], res[NB:])
        g_send[p] = jnp.where(s == 0, res[NB:], res[:NB]).astype(BF16)

    def g_copy(q):
        return pltpu.make_async_remote_copy(
            src_ref=g_send.at[pl.ds(q * CHUNK, CHUNK)], dst_ref=g_recv.at[pl.ds(q * CHUNK, CHUNK)],
            send_sem=g_ssem.at[q], recv_sem=g_rsem.at[q], device_id={"row": partner}, device_id_type=MESH)

    def a_wait(q):
        for slot in range(3):
            a_desc(slot, q, peers[slot], False).wait_recv()

    a_wait(0)
    project(0, 0)

    @pl.loop(0, NCH)
    def _(q):
        @pl.loop(0, CHUNK // 2)
        def _(i):
            p = q * CHUNK + 2 * i

            @pl.when(jnp.logical_and(i == CHUNK // 2 - 1, q < NCH - 1))
            def _():
                a_wait(q + 1)

            project(p + 1, 1)
            attend(p, 0)
            project(jnp.minimum(p + 2, PAIRS - 1), 0)
            attend(p + 1, 1)

        g_copy(q).start()

    for q in range(NCH):
        g_copy(q).wait_recv()

    @pl.loop(0, PAIRS, unroll=4)
    def _(p):
        gf[pl.ds((1 - s) * PAIRS + p, NB, stride=2 * PAIRS), :] = g_recv[p].astype(F32)

    lane_o = lax.broadcasted_iota(jnp.int32, (2 * PAIRS, L), 1)

    @pl.loop(0, NB // 4, unroll=2)
    def _(i4):
        r4 = dot(gf[pl.ds(pl.multiple_of(i4 * 192, 8), 192), :].astype(BF16), wo4[...])
        for k in range(2):
            ra, rb = r4[k * 96:k * 96 + 48], r4[k * 96 + 48:(k + 1) * 96]
            c0 = jnp.where(lane_o < C, ra[:, :L], rb[:, L:])
            c1 = jnp.where(lane_o < C, ra[:, L:], rb[:, :L])
            both = jnp.transpose(jnp.concatenate([c0[:PAIRS], c1[:PAIRS], c0[PAIRS:], c1[PAIRS:]], axis=0))
            i = i4 * 4 + 2 * k
            out_ref[i] = (z_ref[i].astype(F32) + both[:C]).astype(BF16)
            out_ref[i + 1] = (z_ref[i + 1].astype(F32) + both[C:]).astype(BF16)

    for q in range(NCH):
        g_copy(q).wait_send()
        for slot in range(3):
            a_desc(slot, q, peers[slot], False).wait_send()
    for d in range(3):
        z_copy(d).wait_send()
    for u in range(2):
        y_copy(u).wait_send()
        own_copy(u).wait_send()
        fwd_copy(u).wait_send()


def solution(mesh):
    vm = pl.BlockSpec(memory_space=pltpu.VMEM)
    dma = pltpu.SemaphoreType.DMA

    def body(pair_tile, res_mask, ln_gamma, ln_beta, w_q, w_k, w_v, w_b, w_g, w_o):
        out = pl.pallas_call(
            kernel,
            out_shape=jax.ShapeDtypeStruct((NB, C, NB), BF16),
            in_specs=[vm] * 10,
            out_specs=vm,
            scratch_shapes=[
                pltpu.VMEM((NB * 2 * PAIRS, L), F32),
                pltpu.VMEM((NB, 8, L), F32),
                pltpu.VMEM((NB, C, NB), BF16),
                pltpu.VMEM((2 * PAIRS, 3, 32, L), BF16),
                pltpu.VMEM((PAIRS, 3, 4, 32, L), BF16),
                pltpu.VMEM((4, 3, NB, L), BF16),
                pltpu.VMEM((2, 4, 3, NB, L), BF16),
                pltpu.VMEM((HEADS, NQ, NK), F32),
                pltpu.VMEM((2, 2, C, HEADS * NK), BF16),
                pltpu.VMEM((2, HEADS * NK, L), BF16),
                pltpu.VMEM((2, 2, NQ, L), BF16),
                pltpu.VMEM((2, NQ, L), F32),
                pltpu.VMEM((2, NQ, HEADS * NK), BF16),
                pltpu.VMEM((PAIRS, NB, L), BF16),
                pltpu.VMEM((PAIRS, NB, L), BF16),
                pltpu.VMEM((NB * 2 * PAIRS, L), F32),
                pltpu.VMEM((L, L), BF16),
                pltpu.VMEM((L, L), BF16),
                pltpu.VMEM((L, 2 * L), BF16),
                pltpu.VMEM((L, 2 * L), BF16),
                dma((3, NCH)), dma((3, NCH)), dma((3,)), dma((4,)), dma((2,)), dma((2, 2)), dma((2, 4)),
                dma((NCH,)), dma((NCH,)),
            ],
            compiler_params=pltpu.CompilerParams(collective_id=0, has_side_effects=True, vmem_limit_bytes=56 * 2**20),
            name="attend",
        )(jnp.transpose(pair_tile, (0, 2, 1)), res_mask, ln_gamma, ln_beta, w_q, w_k, w_v, w_b.T, w_g, w_o)
        return jnp.transpose(out, (0, 2, 1))

    tile_spec = P(("data", "row"), "col", None)
    return jax.shard_map(body, mesh=mesh, in_specs=(tile_spec, P("data"), P(), P(), P(), P(), P(), P(), P(), P()),
                         out_specs=tile_spec, check_vma=False)
```

```python
import math

import jax
import jax.numpy as jnp
from jax import lax
from jax.experimental import pallas as pl
from jax.experimental.pallas import tpu as pltpu
from jax.sharding import PartitionSpec as P

LN_EPS = 1e-5
MASK_FILL = -1e9
LOG2E = math.log2(math.e)
HEADS = 4
HD = 16
C = 64
NB = 96
NK = 384
NQ = 192
PAIRS = 24
CHUNK = 2
NCH = PAIRS // CHUNK
UNR = 16
UNF = 8
AHEAD = 2
L = 128
MESH = pl.DeviceIdType.MESH
F32 = jnp.float32
BF16 = jnp.bfloat16


def dot(a, b, ca=1, cb=0):
    return lax.dot_general(a, b, (((ca,), (cb,)), ((), ())), preferred_element_type=F32)


def blockdiag2(w):
    z = jnp.zeros_like(w)
    return jnp.concatenate([jnp.concatenate([w, z], 1), jnp.concatenate([z, w], 1)], 0)


def transposed(w):
    return jnp.transpose(w.astype(F32)).astype(BF16)


def down(v, n):
    return jnp.transpose(jnp.broadcast_to(v.reshape(1, n), (L, n)))


def kernel(z_ref, mask_ref, gam_ref, bet_ref, wq_ref, wk_ref, wv_ref, wbt_ref, wg_ref, wo_ref, out_ref,
           t_sc, b_sc, a_own, a_all, bias_z, bias_in, bias_f, kbd, vbd, q_sc, gate_sc, p_sc, g_send, g_recv, gf,
           wk2, wv2, wqg2, wo4,
           a_ssem, a_rsem, z_ssem, z_rsem, y_ssem, f_ssem, b_rsem, g_ssem, g_rsem):
    col = lax.axis_index("col")
    row = lax.axis_index("row")
    y, s = row // 2, lax.rem(row, 2)
    partner = y * 2 + (1 - s)
    across = (1 - y) * 2 + s
    cross = (1 - y) * 2 + (1 - s)
    peers = (partner, across, cross)

    barrier = pltpu.get_barrier_semaphore()
    for r in peers:
        pl.semaphore_signal(barrier, inc=1, device_id={"row": r}, device_id_type=MESH)
    for d in range(1, 4):
        pl.semaphore_signal(barrier, inc=1, device_id={"col": lax.rem(col + d, 4)}, device_id_type=MESH)

    gam = down(gam_ref[...], C)[:, :NB]
    bet = down(bet_ref[...], C)[:, :NB]
    wbt = wbt_ref[...]

    lane_t = lax.broadcasted_iota(jnp.int32, (PAIRS, L), 1)

    def normed(i):
        z = z_ref[i].astype(F32)
        mean = jnp.sum(z, axis=0, keepdims=True) * (1.0 / C)
        cen = z - mean
        var = jnp.sum(cen * cen, axis=0, keepdims=True) * (1.0 / C)
        a = cen * lax.rsqrt(var + LN_EPS) * gam + bet
        b_sc[i, :HEADS, :NB] = dot(wbt, a.astype(BF16))
        return a

    @pl.loop(0, NB // 2, unroll=UNR)
    def _(i2):
        at = jnp.transpose(jnp.concatenate([normed(2 * i2), normed(2 * i2 + 1)], axis=0))
        for half in range(2):
            o = half * 48
            lo, hi = at[o:o + PAIRS], at[o + PAIRS:o + 2 * PAIRS]
            base = pl.multiple_of(i2 * 96 + half * PAIRS, 8)
            t_sc[pl.ds(base, PAIRS), :] = jnp.where(lane_t < C, lo, pltpu.roll(hi, C, 1))
            t_sc[pl.ds(base + 48, PAIRS), :] = jnp.where(lane_t < C, pltpu.roll(lo, C, 1), hi)

    lane = lax.broadcasted_iota(jnp.int32, (NB, L), 1)
    bh = [b_sc.reshape(NB * 8, L)[pl.ds(h, NB, stride=8), :] for h in range(HEADS)]
    for g in range(3):
        bias_z[col, g] = jnp.where(lane < NB, bh[g], pltpu.roll(bh[3], NB - 32 * g, 1)).astype(BF16)

    @pl.loop(0, 2 * PAIRS, unroll=8)
    def _(n):
        a_own[n] = t_sc[pl.ds(n, NB, stride=2 * PAIRS), :].astype(BF16).reshape(3, 32, L)

    pl.semaphore_wait(barrier, 6)

    def z_copy(d):
        return pltpu.make_async_remote_copy(
            src_ref=bias_z.at[col], dst_ref=bias_z.at[col], send_sem=z_ssem.at[d], recv_sem=z_rsem.at[col],
            device_id={"col": lax.rem(col + 1 + d, 4)}, device_id_type=MESH)

    def z_wait(c):
        pltpu.make_async_remote_copy(
            src_ref=bias_z.at[c], dst_ref=bias_z.at[c], send_sem=z_ssem.at[0], recv_sem=z_rsem.at[c],
            device_id={"col": lax.rem(col + 1, 4)}, device_id_type=MESH).wait_recv()

    def bias_copy(src, u, r, ssem, dev):
        return pltpu.make_async_remote_copy(
            src_ref=src, dst_ref=bias_in.at[u, r], send_sem=ssem, recv_sem=b_rsem.at[u, r],
            device_id={"row": dev}, device_id_type=MESH)

    def y_copy(u):
        return bias_copy(bias_z.at[2 * (1 - y) + u], u, row, y_ssem.at[u], across)

    def own_copy(u):
        return bias_copy(bias_z.at[2 * y + u], u, row, f_ssem.at[u, 0], partner)

    def fwd_copy(u):
        return bias_copy(bias_in.at[u, across], u, across, f_ssem.at[u, 1], partner)

    def bias_wait(u, r):
        bias_copy(bias_in.at[u, r], u, r, y_ssem.at[u], partner).wait_recv()

    for d in range(3):
        z_copy(d).start()

    def a_desc(slot, q, r, last):
        dst = a_all.at[pl.ds(q * CHUNK, CHUNK), :, 3] if last else a_all.at[pl.ds(q * CHUNK, CHUNK), jnp.minimum(row, 2), 0:3]
        return pltpu.make_async_remote_copy(
            src_ref=a_own.at[pl.ds(lax.rem(r, 2) * PAIRS + q * CHUNK, CHUNK)], dst_ref=dst,
            send_sem=a_ssem.at[slot, q], recv_sem=a_rsem.at[slot, q],
            device_id={"row": r}, device_id_type=MESH)

    def a_start(slot, q):
        @pl.when(row == 3)
        def _():
            a_desc(slot, q, peers[slot], True).start()

        @pl.when(row < 3)
        def _():
            a_desc(slot, q, peers[slot], False).start()

    for q in range(AHEAD):
        for slot in (1, 2, 0):
            a_start(slot, q)

    @pl.when(row == 3)
    def _():
        a_all[:, :, 3] = a_own[pl.ds(s * PAIRS, PAIRS)]

    @pl.when(row < 3)
    def _():
        a_all[:, jnp.minimum(row, 2), 0:3] = a_own[pl.ds(s * PAIRS, PAIRS)]

    wk2[...] = blockdiag2(transposed(wk_ref[...]))
    wv2[...] = blockdiag2(wv_ref[...])
    wqg2[:, :L] = blockdiag2(wq_ref[...])
    wqg2[:, L:] = blockdiag2(wg_ref[...])
    wo = wo_ref[...]
    wo4[:, :L] = blockdiag2(wo)
    wo4[:, L:] = jnp.concatenate([jnp.concatenate([jnp.zeros_like(wo), wo], 1), jnp.concatenate([wo, jnp.zeros_like(wo)], 1)], 0)
    for par in range(2):
        for t in range(2):
            kbd[par, t] = jnp.zeros((C, HEADS * NK), BF16)

    for u in range(2):
        @pl.when(2 * (1 - y) + u != col)
        def _(u=u):
            z_wait(2 * (1 - y) + u)
        y_copy(u).start()
    for q in range(AHEAD, NCH):
        for slot in (1, 2, 0):
            a_start(slot, q)
    for u in range(2):
        @pl.when(2 * y + u != col)
        def _(u=u):
            z_wait(2 * y + u)
        own_copy(u).start()
        bias_in[u, row] = bias_z[2 * y + u]
    for u in range(2):
        bias_wait(u, across)
        fwd_copy(u).start()
    for u in range(2):
        for r in (partner, cross):
            bias_wait(u, r)

    fill = down(jnp.where(mask_ref[...] > 0, 0.0, MASK_FILL).astype(F32), NK)
    for u in range(2):
        for g in range(3):
            parts = []
            for t in range(3):
                parts.append(bias_in[u, t, g].astype(F32) + fill[t * NB:(t + 1) * NB])
                parts.append(bias_in[u, 3, g, t * 32:(t + 1) * 32].astype(F32) + fill[3 * NB + t * 32:3 * NB + (t + 1) * 32])
            bt = jnp.transpose(jnp.concatenate(parts, axis=0)) * LOG2E
            bias_f[g, u * NB:(u + 1) * NB, :] = bt[:NB]
            bias_f[3, u * NB + g * 32:u * NB + (g + 1) * 32, :] = bt[NB:]

    hid = lax.rem(lax.broadcasted_iota(jnp.int32, (NK, L), 1), C) // HD
    lane_q = lax.broadcasted_iota(jnp.int32, (NQ, L), 1)
    hid_q = lax.rem(lane_q, C) // HD

    def project(p, par):
        x = a_all[p].reshape(NK, L)
        x_lo = a_all[p, 0:2, 0:3].reshape(NQ, L)
        x_hi = jnp.concatenate([a_all[p, 2, 0:3].reshape(NB, L), a_all[p, :, 3].reshape(NB, L)], axis=0)
        qg = dot(jnp.where(y == 0, x_lo, x_hi), wqg2[...])
        v2 = dot(x, wv2[...]).astype(BF16)
        kt = dot(wk2[...], x, 1, 1).astype(BF16)
        gate_sc[par] = jax.nn.sigmoid(qg[:, L:])
        q2 = (qg[:, :L] * (1.0 / math.sqrt(HD))).astype(BF16)
        for h in range(HEADS):
            vbd[par, h * NK:(h + 1) * NK, :] = jnp.where(hid == h, v2, jnp.zeros_like(v2))
        for t in range(2):
            q_sc[par, t, :, :C] = q2[:, t * C:(t + 1) * C]
            for h in range(HEADS):
                kbd[par, t, h * HD:(h + 1) * HD, h * NK:(h + 1) * NK] = kt[t * C + h * HD:t * C + (h + 1) * HD, :]

    def softmax(t, logits):
        sums = []
        for h in range(HEADS):
            lt = logits[:, h * NK:(h + 1) * NK] * LOG2E + bias_f[h]
            e = jnp.exp2(lt - jnp.max(lt, axis=1, keepdims=True))
            sums.append(jnp.sum(e, axis=1, keepdims=True))
            p_sc[t, :, h * NK:(h + 1) * NK] = e.astype(BF16)
        return sums

    def attend(p, par):
        logits = [dot(q_sc[par, t, :, :C], kbd[par, t]) for t in range(2)]
        sums = [softmax(t, logits[t]) for t in range(2)]
        o = []
        for t in range(2):
            l = sums[t]
            div = jnp.where(hid_q == 0, l[0], jnp.where(hid_q == 1, l[1], jnp.where(hid_q == 2, l[2], l[3])))
            o.append(dot(p_sc[t], vbd[par]) / div)
        res = gate_sc[par] * jnp.where(lane_q < C, o[0], o[1])
        gf[pl.ds(s * PAIRS + p, NB, stride=2 * PAIRS), :] = jnp.where(s == 0, res[:NB], res[NB:])
        g_send[p] = jnp.where(s == 0, res[NB:], res[:NB]).astype(BF16)

    def g_copy(q):
        return pltpu.make_async_remote_copy(
            src_ref=g_send.at[pl.ds(q * CHUNK, CHUNK)], dst_ref=g_recv.at[pl.ds(q * CHUNK, CHUNK)],
            send_sem=g_ssem.at[q], recv_sem=g_rsem.at[q], device_id={"row": partner}, device_id_type=MESH)

    def a_wait(q):
        for slot in range(3):
            a_desc(slot, q, peers[slot], False).wait_recv()

    a_wait(0)
    project(0, 0)

    @pl.loop(0, NCH)
    def _(q):
        @pl.loop(0, CHUNK // 2)
        def _(i):
            p = q * CHUNK + 2 * i

            @pl.when(jnp.logical_and(i == CHUNK // 2 - 1, q < NCH - 1))
            def _():
                a_wait(q + 1)

            project(p + 1, 1)
            attend(p, 0)
            project(jnp.minimum(p + 2, PAIRS - 1), 0)
            attend(p + 1, 1)

        g_copy(q).start()

    for q in range(NCH):
        g_copy(q).wait_recv()

    @pl.loop(0, PAIRS, unroll=4)
    def _(p):
        gf[pl.ds((1 - s) * PAIRS + p, NB, stride=2 * PAIRS), :] = g_recv[p].astype(F32)

    lane_o = lax.broadcasted_iota(jnp.int32, (2 * PAIRS, L), 1)

    @pl.loop(0, NB // 4, unroll=UNF)
    def _(i4):
        r4 = dot(gf[pl.ds(pl.multiple_of(i4 * 192, 8), 192), :].astype(BF16), wo4[...])
        for k in range(2):
            ra, rb = r4[k * 96:k * 96 + 48], r4[k * 96 + 48:(k + 1) * 96]
            c0 = jnp.where(lane_o < C, ra[:, :L], rb[:, L:])
            c1 = jnp.where(lane_o < C, ra[:, L:], rb[:, :L])
            both = jnp.transpose(jnp.concatenate([c0[:PAIRS], c1[:PAIRS], c0[PAIRS:], c1[PAIRS:]], axis=0))
            i = i4 * 4 + 2 * k
            out_ref[i] = (z_ref[i].astype(F32) + both[:C]).astype(BF16)
            out_ref[i + 1] = (z_ref[i + 1].astype(F32) + both[C:]).astype(BF16)

    for q in range(NCH):
        g_copy(q).wait_send()
        for slot in range(3):
            a_desc(slot, q, peers[slot], False).wait_send()
    for d in range(3):
        z_copy(d).wait_send()
    for u in range(2):
        y_copy(u).wait_send()
        own_copy(u).wait_send()
        fwd_copy(u).wait_send()


def solution(mesh):
    vm = pl.BlockSpec(memory_space=pltpu.VMEM)
    dma = pltpu.SemaphoreType.DMA

    def body(pair_tile, res_mask, ln_gamma, ln_beta, w_q, w_k, w_v, w_b, w_g, w_o):
        out = pl.pallas_call(
            kernel,
            out_shape=jax.ShapeDtypeStruct((NB, C, NB), BF16),
            in_specs=[vm] * 10,
            out_specs=vm,
            scratch_shapes=[
                pltpu.VMEM((NB * 2 * PAIRS, L), F32),
                pltpu.VMEM((NB, 8, L), F32),
                pltpu.VMEM((2 * PAIRS, 3, 32, L), BF16),
                pltpu.VMEM((PAIRS, 3, 4, 32, L), BF16),
                pltpu.VMEM((4, 3, NB, L), BF16),
                pltpu.VMEM((2, 4, 3, NB, L), BF16),
                pltpu.VMEM((HEADS, NQ, NK), F32),
                pltpu.VMEM((2, 2, C, HEADS * NK), BF16),
                pltpu.VMEM((2, HEADS * NK, L), BF16),
                pltpu.VMEM((2, 2, NQ, L), BF16),
                pltpu.VMEM((2, NQ, L), F32),
                pltpu.VMEM((2, NQ, HEADS * NK), BF16),
                pltpu.VMEM((PAIRS, NB, L), BF16),
                pltpu.VMEM((PAIRS, NB, L), BF16),
                pltpu.VMEM((NB * 2 * PAIRS, L), F32),
                pltpu.VMEM((L, L), BF16),
                pltpu.VMEM((L, L), BF16),
                pltpu.VMEM((L, 2 * L), BF16),
                pltpu.VMEM((L, 2 * L), BF16),
                dma((3, NCH)), dma((3, NCH)), dma((3,)), dma((4,)), dma((2,)), dma((2, 2)), dma((2, 4)),
                dma((NCH,)), dma((NCH,)),
            ],
            compiler_params=pltpu.CompilerParams(collective_id=0, has_side_effects=True, vmem_limit_bytes=56 * 2**20),
            name="attend",
        )(jnp.transpose(pair_tile, (0, 2, 1)), res_mask, ln_gamma, ln_beta, w_q, w_k, w_v, w_b.T, w_g, w_o)
        return jnp.transpose(out, (0, 2, 1))

    tile_spec = P(("data", "row"), "col", None)
    return jax.shard_map(body, mesh=mesh, in_specs=(tile_spec, P("data"), P(), P(), P(), P(), P(), P(), P(), P()),
                         out_specs=tile_spec, check_vma=False)
```

```python
import math

import jax
import jax.numpy as jnp
from jax import lax
from jax.experimental import pallas as pl
from jax.experimental.pallas import tpu as pltpu
from jax.sharding import PartitionSpec as P

LN_EPS = 1e-5
MASK_FILL = -1e9
LOG2E = math.log2(math.e)
HEADS = 4
HD = 16
C = 64
NB = 96
NK = 384
NQ = 192
PAIRS = 24
CHUNK = 2
NCH = PAIRS // CHUNK
UNR = 16
STEP = 48
AHEAD = 2
L = 128
MESH = pl.DeviceIdType.MESH
F32 = jnp.float32
BF16 = jnp.bfloat16


def dot(a, b, ca=1, cb=0):
    return lax.dot_general(a, b, (((ca,), (cb,)), ((), ())), preferred_element_type=F32)


def blockdiag2(w):
    z = jnp.zeros_like(w)
    return jnp.concatenate([jnp.concatenate([w, z], 1), jnp.concatenate([z, w], 1)], 0)


def transposed(w):
    return jnp.transpose(w.astype(F32)).astype(BF16)


def down(v, n):
    return jnp.transpose(jnp.broadcast_to(v.reshape(1, n), (L, n)))


def kernel(z_ref, mask_ref, gam_ref, bet_ref, wq_ref, wk_ref, wv_ref, wbt_ref, wg_ref, out_ref,
           t_sc, b_sc, a_own, a_all, bias_z, bias_in, bias_f, kbd, vbd, q_sc, gate_sc, p_sc, g_send, g_recv, gf,
           wk2, wv2, wqg2,
           a_ssem, a_rsem, z_ssem, z_rsem, y_ssem, f_ssem, b_rsem, g_ssem, g_rsem):
    col = lax.axis_index("col")
    row = lax.axis_index("row")
    y, s = row // 2, lax.rem(row, 2)
    partner = y * 2 + (1 - s)
    across = (1 - y) * 2 + s
    cross = (1 - y) * 2 + (1 - s)
    peers = (partner, across, cross)

    barrier = pltpu.get_barrier_semaphore()
    for r in peers:
        pl.semaphore_signal(barrier, inc=1, device_id={"row": r}, device_id_type=MESH)
    for d in range(1, 4):
        pl.semaphore_signal(barrier, inc=1, device_id={"col": lax.rem(col + d, 4)}, device_id_type=MESH)

    gam = down(gam_ref[...], C)[:, :NB]
    bet = down(bet_ref[...], C)[:, :NB]
    wbt = wbt_ref[...]

    lane_t = lax.broadcasted_iota(jnp.int32, (PAIRS, L), 1)

    def normed(i):
        z = z_ref[i].astype(F32)
        mean = jnp.sum(z, axis=0, keepdims=True) * (1.0 / C)
        cen = z - mean
        var = jnp.sum(cen * cen, axis=0, keepdims=True) * (1.0 / C)
        a = cen * lax.rsqrt(var + LN_EPS) * gam + bet
        b_sc[i, :HEADS, :NB] = dot(wbt, a.astype(BF16))
        return a

    @pl.loop(0, NB // 2, unroll=UNR)
    def _(i2):
        at = jnp.transpose(jnp.concatenate([normed(2 * i2), normed(2 * i2 + 1)], axis=0))
        for half in range(2):
            o = half * 48
            lo, hi = at[o:o + PAIRS], at[o + PAIRS:o + 2 * PAIRS]
            base = pl.multiple_of(i2 * 96 + half * PAIRS, 8)
            t_sc[pl.ds(base, PAIRS), :] = jnp.where(lane_t < C, lo, pltpu.roll(hi, C, 1))
            t_sc[pl.ds(base + 48, PAIRS), :] = jnp.where(lane_t < C, pltpu.roll(lo, C, 1), hi)

    lane = lax.broadcasted_iota(jnp.int32, (NB, L), 1)
    bh = [b_sc.reshape(NB * 8, L)[pl.ds(h, NB, stride=8), :] for h in range(HEADS)]
    for g in range(3):
        bias_z[col, g] = jnp.where(lane < NB, bh[g], pltpu.roll(bh[3], NB - 32 * g, 1)).astype(BF16)

    pl.semaphore_wait(barrier, 6)

    def z_dest(k):
        return jnp.where(col < 2, 3 - k, k)

    def z_copy(k):
        return pltpu.make_async_remote_copy(
            src_ref=bias_z.at[col], dst_ref=bias_z.at[col], send_sem=z_ssem.at[k], recv_sem=z_rsem.at[col],
            device_id={"col": z_dest(k)}, device_id_type=MESH)

    def z_wait(c):
        pltpu.make_async_remote_copy(
            src_ref=bias_z.at[c], dst_ref=bias_z.at[c], send_sem=z_ssem.at[0], recv_sem=z_rsem.at[c],
            device_id={"col": lax.rem(col + 1, 4)}, device_id_type=MESH).wait_recv()

    def bias_copy(src, u, r, ssem, dev):
        return pltpu.make_async_remote_copy(
            src_ref=src, dst_ref=bias_in.at[u, r], send_sem=ssem, recv_sem=b_rsem.at[u, r],
            device_id={"row": dev}, device_id_type=MESH)

    def y_copy(u):
        return bias_copy(bias_z.at[2 * (1 - y) + u], u, row, y_ssem.at[u], across)

    def own_copy(u):
        return bias_copy(bias_z.at[2 * y + u], u, row, f_ssem.at[u, 0], partner)

    def fwd_copy(u):
        return bias_copy(bias_in.at[u, across], u, across, f_ssem.at[u, 1], partner)

    def bias_wait(u, r):
        bias_copy(bias_in.at[u, r], u, r, y_ssem.at[u], partner).wait_recv()

    for k in range(4):
        @pl.when(z_dest(k) != col)
        def _(k=k):
            z_copy(k).start()

    @pl.loop(0, 2 * PAIRS, unroll=8)
    def _(n):
        a_own[n] = t_sc[pl.ds(n, NB, stride=2 * PAIRS), :].astype(BF16).reshape(3, 32, L)

    def a_desc(slot, q, r, last):
        dst = a_all.at[pl.ds(q * CHUNK, CHUNK), :, 3] if last else a_all.at[pl.ds(q * CHUNK, CHUNK), jnp.minimum(row, 2), 0:3]
        return pltpu.make_async_remote_copy(
            src_ref=a_own.at[pl.ds(lax.rem(r, 2) * PAIRS + q * CHUNK, CHUNK)], dst_ref=dst,
            send_sem=a_ssem.at[slot, q], recv_sem=a_rsem.at[slot, q],
            device_id={"row": r}, device_id_type=MESH)

    def a_start(slot, q):
        @pl.when(row == 3)
        def _():
            a_desc(slot, q, peers[slot], True).start()

        @pl.when(row < 3)
        def _():
            a_desc(slot, q, peers[slot], False).start()

    for q in range(AHEAD):
        for slot in (1, 2, 0):
            a_start(slot, q)

    @pl.when(row == 3)
    def _():
        a_all[:, :, 3] = a_own[pl.ds(s * PAIRS, PAIRS)]

    @pl.when(row < 3)
    def _():
        a_all[:, jnp.minimum(row, 2), 0:3] = a_own[pl.ds(s * PAIRS, PAIRS)]

    wk2[...] = blockdiag2(transposed(wk_ref[...]))
    wv2[...] = blockdiag2(wv_ref[...])
    wqg2[:, :L] = blockdiag2(wq_ref[...])
    wqg2[:, L:] = blockdiag2(wg_ref[...])
    for par in range(2):
        for t in range(2):
            kbd[par, t] = jnp.zeros((C, HEADS * NK), BF16)

    for u in range(2):
        @pl.when(2 * (1 - y) + u != col)
        def _(u=u):
            z_wait(2 * (1 - y) + u)
        y_copy(u).start()
    for q in range(AHEAD, NCH):
        for slot in (1, 2, 0):
            a_start(slot, q)
    for u in range(2):
        @pl.when(2 * y + u != col)
        def _(u=u):
            z_wait(2 * y + u)
        own_copy(u).start()
        bias_in[u, row] = bias_z[2 * y + u]
    for u in range(2):
        bias_wait(u, across)
        fwd_copy(u).start()
    fill = down(jnp.where(mask_ref[...] > 0, 0.0, MASK_FILL).astype(F32), NK)
    for u in range(2):
        bias_wait(u, partner)
        bias_wait(u, cross)
        for g in range(3):
            parts = []
            for t in range(3):
                parts.append(bias_in[u, t, g].astype(F32) + fill[t * NB:(t + 1) * NB])
                parts.append(bias_in[u, 3, g, t * 32:(t + 1) * 32].astype(F32) + fill[3 * NB + t * 32:3 * NB + (t + 1) * 32])
            bt = jnp.transpose(jnp.concatenate(parts, axis=0)) * LOG2E
            bias_f[g, u * NB:(u + 1) * NB, :] = bt[:NB]
            bias_f[3, u * NB + g * 32:u * NB + (g + 1) * 32, :] = bt[NB:]

    hid = lax.rem(lax.broadcasted_iota(jnp.int32, (NK, L), 1), C) // HD
    lane_q = lax.broadcasted_iota(jnp.int32, (NQ, L), 1)
    hid_q = lax.rem(lane_q, C) // HD

    def project(p, par):
        x = a_all[p].reshape(NK, L)
        x_lo = a_all[p, 0:2, 0:3].reshape(NQ, L)
        x_hi = jnp.concatenate([a_all[p, 2, 0:3].reshape(NB, L), a_all[p, :, 3].reshape(NB, L)], axis=0)
        qg = dot(jnp.where(y == 0, x_lo, x_hi), wqg2[...])
        v2 = dot(x, wv2[...]).astype(BF16)
        kt = dot(wk2[...], x, 1, 1).astype(BF16)
        gate_sc[par] = jax.nn.sigmoid(qg[:, L:])
        q2 = (qg[:, :L] * (1.0 / math.sqrt(HD))).astype(BF16)
        for h in range(HEADS):
            vbd[par, h * NK:(h + 1) * NK, :] = jnp.where(hid == h, v2, jnp.zeros_like(v2))
        for t in range(2):
            q_sc[par, t, :, :C] = q2[:, t * C:(t + 1) * C]
            for h in range(HEADS):
                kbd[par, t, h * HD:(h + 1) * HD, h * NK:(h + 1) * NK] = kt[t * C + h * HD:t * C + (h + 1) * HD, :]

    def softmax(t, logits):
        sums = []
        for h in range(HEADS):
            lt = logits[:, h * NK:(h + 1) * NK] * LOG2E + bias_f[h]
            e = jnp.exp2(lt - jnp.max(lt, axis=1, keepdims=True))
            sums.append(jnp.sum(e, axis=1, keepdims=True))
            p_sc[t, :, h * NK:(h + 1) * NK] = e.astype(BF16)
        return sums

    def attend(p, par):
        logits = [dot(q_sc[par, t, :, :C], kbd[par, t]) for t in range(2)]
        sums = [softmax(t, logits[t]) for t in range(2)]
        o = []
        for t in range(2):
            l = sums[t]
            div = jnp.where(hid_q == 0, l[0], jnp.where(hid_q == 1, l[1], jnp.where(hid_q == 2, l[2], l[3])))
            o.append(dot(p_sc[t], vbd[par]) / div)
        res = gate_sc[par] * jnp.where(lane_q < C, o[0], o[1])
        gf[pl.ds(s * PAIRS + p, NB, stride=2 * PAIRS), :] = jnp.where(s == 0, res[:NB], res[NB:])
        g_send[p] = jnp.where(s == 0, res[NB:], res[:NB]).astype(BF16)

    def g_copy(q):
        return pltpu.make_async_remote_copy(
            src_ref=g_send.at[pl.ds(q * CHUNK, CHUNK)], dst_ref=g_recv.at[pl.ds(q * CHUNK, CHUNK)],
            send_sem=g_ssem.at[q], recv_sem=g_rsem.at[q], device_id={"row": partner}, device_id_type=MESH)

    def a_wait(q):
        for slot in range(3):
            a_desc(slot, q, peers[slot], False).wait_recv()

    a_wait(0)
    project(0, 0)

    @pl.loop(0, NCH)
    def _(q):
        @pl.loop(0, CHUNK // 2)
        def _(i):
            p = q * CHUNK + 2 * i

            @pl.when(jnp.logical_and(i == CHUNK // 2 - 1, q < NCH - 1))
            def _():
                a_wait(q + 1)

            project(p + 1, 1)
            attend(p, 0)
            project(jnp.minimum(p + 2, PAIRS - 1), 0)
            attend(p + 1, 1)

        g_copy(q).start()

    for q in range(NCH):
        g_copy(q).wait_recv()

    @pl.loop(0, PAIRS, unroll=4)
    def _(p):
        gf[pl.ds((1 - s) * PAIRS + p, NB, stride=2 * PAIRS), :] = g_recv[p].astype(F32)

    @pl.loop(0, NB // 4, unroll=8)
    def _(i4):
        rows = pl.ds(pl.multiple_of(i4 * 192, 64), 192)
        out_ref[rows, :] = gf[rows, :].astype(BF16)

    for q in range(NCH):
        g_copy(q).wait_send()
        for slot in range(3):
            a_desc(slot, q, peers[slot], False).wait_send()
    for k in range(4):
        @pl.when(z_dest(k) != col)
        def _(k=k):
            z_copy(k).wait_send()
    for u in range(2):
        y_copy(u).wait_send()
        own_copy(u).wait_send()
        fwd_copy(u).wait_send()


def project_out(gated_ref, z_ref, wo_ref, out_ref):
    wo = wo_ref[...]
    zero = jnp.zeros_like(wo)
    swapped = jnp.concatenate([jnp.concatenate([zero, wo], 1), jnp.concatenate([wo, zero], 1)], 0)
    wo4 = jnp.concatenate([blockdiag2(wo), swapped], axis=1)
    lane_o = lax.broadcasted_iota(jnp.int32, (2 * PAIRS, L), 1)
    for i4 in range(STEP // 4):
        r4 = dot(gated_ref[i4 * 192:(i4 + 1) * 192, :], wo4)
        for k in range(2):
            ra, rb = r4[k * 96:k * 96 + 48], r4[k * 96 + 48:(k + 1) * 96]
            c0 = jnp.where(lane_o < C, ra[:, :L], rb[:, L:])
            c1 = jnp.where(lane_o < C, ra[:, L:], rb[:, :L])
            both = jnp.transpose(jnp.concatenate([c0[:PAIRS], c1[:PAIRS], c0[PAIRS:], c1[PAIRS:]], axis=0))
            i = i4 * 4 + 2 * k
            out_ref[i] = (z_ref[i].astype(F32) + both[:C]).astype(BF16)
            out_ref[i + 1] = (z_ref[i + 1].astype(F32) + both[C:]).astype(BF16)


def solution(mesh):
    vm = pl.BlockSpec(memory_space=pltpu.VMEM)
    dma = pltpu.SemaphoreType.DMA

    def body(pair_tile, res_mask, ln_gamma, ln_beta, w_q, w_k, w_v, w_b, w_g, w_o):
        z_t = jnp.transpose(pair_tile, (0, 2, 1))
        gated = pl.pallas_call(
            kernel,
            out_shape=jax.ShapeDtypeStruct((NB * 2 * PAIRS, L), BF16),
            in_specs=[vm] * 9,
            out_specs=vm,
            scratch_shapes=[
                pltpu.VMEM((NB * 2 * PAIRS, L), F32),
                pltpu.VMEM((NB, 8, L), F32),
                pltpu.VMEM((2 * PAIRS, 3, 32, L), BF16),
                pltpu.VMEM((PAIRS, 3, 4, 32, L), BF16),
                pltpu.VMEM((4, 3, NB, L), BF16),
                pltpu.VMEM((2, 4, 3, NB, L), BF16),
                pltpu.VMEM((HEADS, NQ, NK), F32),
                pltpu.VMEM((2, 2, C, HEADS * NK), BF16),
                pltpu.VMEM((2, HEADS * NK, L), BF16),
                pltpu.VMEM((2, 2, NQ, L), BF16),
                pltpu.VMEM((2, NQ, L), F32),
                pltpu.VMEM((2, NQ, HEADS * NK), BF16),
                pltpu.VMEM((PAIRS, NB, L), BF16),
                pltpu.VMEM((PAIRS, NB, L), BF16),
                pltpu.VMEM((NB * 2 * PAIRS, L), F32),
                pltpu.VMEM((L, L), BF16),
                pltpu.VMEM((L, L), BF16),
                pltpu.VMEM((L, 2 * L), BF16),
                dma((3, NCH)), dma((3, NCH)), dma((4,)), dma((4,)), dma((2,)), dma((2, 2)), dma((2, 4)),
                dma((NCH,)), dma((NCH,)),
            ],
            compiler_params=pltpu.CompilerParams(collective_id=0, has_side_effects=True, vmem_limit_bytes=56 * 2**20),
            name="attend",
        )(z_t, res_mask, ln_gamma, ln_beta, w_q, w_k, w_v, w_b.T, w_g)
        tile = pl.BlockSpec((STEP, C, NB), lambda n: (n, 0, 0))
        out = pl.pallas_call(
            project_out,
            out_shape=jax.ShapeDtypeStruct((NB, C, NB), BF16),
            grid=(NB // STEP,),
            in_specs=[pl.BlockSpec((STEP * 2 * PAIRS, L), lambda n: (n, 0)), tile, pl.BlockSpec((C, C), lambda n: (0, 0))],
            out_specs=tile,
            name="project_out",
        )(gated, z_t, w_o)
        return jnp.transpose(out, (0, 2, 1))

    tile_spec = P(("data", "row"), "col", None)
    return jax.shard_map(body, mesh=mesh, in_specs=(tile_spec, P("data"), P(), P(), P(), P(), P(), P(), P(), P()),
                         out_specs=tile_spec, check_vma=False)
```

```python
import math

import jax
import jax.numpy as jnp
from jax import lax
from jax.experimental import pallas as pl
from jax.experimental.pallas import tpu as pltpu
from jax.sharding import PartitionSpec as P

LN_EPS = 1e-5
MASK_FILL = -1e9
LOG2E = math.log2(math.e)
HEADS = 4
HD = 16
C = 64
NB = 96
NK = 384
NQ = 192
PAIRS = 24
CHUNK = 2
NCH = PAIRS // CHUNK
UNR = 16
STEP = 48
AHEAD = 2
L = 128
MESH = pl.DeviceIdType.MESH
F32 = jnp.float32
BF16 = jnp.bfloat16


def dot(a, b, ca=1, cb=0):
    return lax.dot_general(a, b, (((ca,), (cb,)), ((), ())), preferred_element_type=F32)


def blockdiag2(w):
    z = jnp.zeros_like(w)
    return jnp.concatenate([jnp.concatenate([w, z], 1), jnp.concatenate([z, w], 1)], 0)


def transposed(w):
    return jnp.transpose(w.astype(F32)).astype(BF16)


def down(v, n):
    return jnp.transpose(jnp.broadcast_to(v.reshape(1, n), (L, n)))


def kernel(z_ref, mask_ref, gam_ref, bet_ref, wq_ref, wk_ref, wv_ref, wbt_ref, wg_ref, out_ref,
           t_sc, b_sc, a_own, a_all, bias_z, bias_in, bias_f, kbd, vbd, q_sc, gate_sc, p_sc, g_send, g_recv, gf,
           wk2, wv2, wqg2,
           a_ssem, a_rsem, z_ssem, z_rsem, y_ssem, f_ssem, b_rsem, g_ssem, g_rsem):
    col = lax.axis_index("col")
    row = lax.axis_index("row")
    y, s = row // 2, lax.rem(row, 2)
    partner = y * 2 + (1 - s)
    across = (1 - y) * 2 + s
    cross = (1 - y) * 2 + (1 - s)
    peers = (partner, across, cross)

    barrier = pltpu.get_barrier_semaphore()
    for r in peers:
        pl.semaphore_signal(barrier, inc=1, device_id={"row": r}, device_id_type=MESH)
    for d in range(1, 4):
        pl.semaphore_signal(barrier, inc=1, device_id={"col": lax.rem(col + d, 4)}, device_id_type=MESH)

    gam = down(gam_ref[...], C)[:, :NB]
    bet = down(bet_ref[...], C)[:, :NB]
    wbt = wbt_ref[...]

    lane_t = lax.broadcasted_iota(jnp.int32, (PAIRS, L), 1)

    def normed(i):
        z = z_ref[i].astype(F32)
        mean = jnp.sum(z, axis=0, keepdims=True) * (1.0 / C)
        cen = z - mean
        var = jnp.sum(cen * cen, axis=0, keepdims=True) * (1.0 / C)
        a = cen * lax.rsqrt(var + LN_EPS) * gam + bet
        b_sc[i, :HEADS, :NB] = dot(wbt, a.astype(BF16))
        return a

    @pl.loop(0, NB // 2, unroll=UNR)
    def _(i2):
        at = jnp.transpose(jnp.concatenate([normed(2 * i2), normed(2 * i2 + 1)], axis=0))
        for half in range(2):
            o = half * 48
            lo, hi = at[o:o + PAIRS], at[o + PAIRS:o + 2 * PAIRS]
            base = pl.multiple_of(i2 * 96 + half * PAIRS, 8)
            t_sc[pl.ds(base, PAIRS), :] = jnp.where(lane_t < C, lo, pltpu.roll(hi, C, 1))
            t_sc[pl.ds(base + 48, PAIRS), :] = jnp.where(lane_t < C, pltpu.roll(lo, C, 1), hi)

    lane = lax.broadcasted_iota(jnp.int32, (NB, L), 1)
    bh = [b_sc.reshape(NB * 8, L)[pl.ds(h, NB, stride=8), :] for h in range(HEADS)]
    for g in range(3):
        bias_z[col, g] = jnp.where(lane < NB, bh[g], pltpu.roll(bh[3], NB - 32 * g, 1)).astype(BF16)

    pl.semaphore_wait(barrier, 6)

    def z_dest(k):
        return jnp.where(col < 2, 3 - k, k)

    def z_copy(k):
        return pltpu.make_async_remote_copy(
            src_ref=bias_z.at[col], dst_ref=bias_z.at[col], send_sem=z_ssem.at[k], recv_sem=z_rsem.at[col],
            device_id={"col": z_dest(k)}, device_id_type=MESH)

    def z_wait(c):
        pltpu.make_async_remote_copy(
            src_ref=bias_z.at[c], dst_ref=bias_z.at[c], send_sem=z_ssem.at[0], recv_sem=z_rsem.at[c],
            device_id={"col": lax.rem(col + 1, 4)}, device_id_type=MESH).wait_recv()

    def bias_copy(src, u, r, ssem, dev):
        return pltpu.make_async_remote_copy(
            src_ref=src, dst_ref=bias_in.at[u, r], send_sem=ssem, recv_sem=b_rsem.at[u, r],
            device_id={"row": dev}, device_id_type=MESH)

    def y_copy(u):
        return bias_copy(bias_z.at[2 * (1 - y) + u], u, row, y_ssem.at[u], across)

    def own_copy(u):
        return bias_copy(bias_z.at[2 * y + u], u, row, f_ssem.at[u, 0], partner)

    def fwd_copy(u):
        return bias_copy(bias_in.at[u, across], u, across, f_ssem.at[u, 1], partner)

    def bias_wait(u, r):
        bias_copy(bias_in.at[u, r], u, r, y_ssem.at[u], partner).wait_recv()

    for k in range(4):
        @pl.when(z_dest(k) != col)
        def _(k=k):
            z_copy(k).start()

    @pl.loop(0, 2 * PAIRS, unroll=8)
    def _(n):
        a_own[n] = t_sc[pl.ds(n, NB, stride=2 * PAIRS), :].astype(BF16).reshape(3, 32, L)

    def a_desc(slot, q, r, last):
        dst = a_all.at[pl.ds(q * CHUNK, CHUNK), :, 3] if last else a_all.at[pl.ds(q * CHUNK, CHUNK), jnp.minimum(row, 2), 0:3]
        return pltpu.make_async_remote_copy(
            src_ref=a_own.at[pl.ds(lax.rem(r, 2) * PAIRS + q * CHUNK, CHUNK)], dst_ref=dst,
            send_sem=a_ssem.at[slot, q], recv_sem=a_rsem.at[slot, q],
            device_id={"row": r}, device_id_type=MESH)

    def a_start(slot, q):
        @pl.when(row == 3)
        def _():
            a_desc(slot, q, peers[slot], True).start()

        @pl.when(row < 3)
        def _():
            a_desc(slot, q, peers[slot], False).start()

    for q in range(AHEAD):
        for slot in (1, 2, 0):
            a_start(slot, q)

    @pl.when(row == 3)
    def _():
        a_all[:, :, 3] = a_own[pl.ds(s * PAIRS, PAIRS)]

    @pl.when(row < 3)
    def _():
        a_all[:, jnp.minimum(row, 2), 0:3] = a_own[pl.ds(s * PAIRS, PAIRS)]

    wk2[...] = blockdiag2(transposed(wk_ref[...]))
    wv2[...] = blockdiag2(wv_ref[...])
    wqg2[:, :L] = blockdiag2(wq_ref[...])
    wqg2[:, L:] = blockdiag2(wg_ref[...])
    for par in range(CHUNK * AHEAD):
        for t in range(2):
            kbd[par, t] = jnp.zeros((C, HEADS * NK), BF16)

    for u in range(2):
        @pl.when(2 * (1 - y) + u != col)
        def _(u=u):
            z_wait(2 * (1 - y) + u)
        y_copy(u).start()
    for q in range(AHEAD, NCH):
        for slot in (1, 2, 0):
            a_start(slot, q)
    for u in range(2):
        @pl.when(2 * y + u != col)
        def _(u=u):
            z_wait(2 * y + u)
        own_copy(u).start()
        bias_in[u, row] = bias_z[2 * y + u]
    def a_wait(q):
        for slot in range(3):
            a_desc(slot, q, peers[slot], False).wait_recv()

    hid = lax.rem(lax.broadcasted_iota(jnp.int32, (NK, L), 1), C) // HD
    lane_q = lax.broadcasted_iota(jnp.int32, (NQ, L), 1)
    hid_q = lax.rem(lane_q, C) // HD

    def project(p, par):
        x = a_all[p].reshape(NK, L)
        x_lo = a_all[p, 0:2, 0:3].reshape(NQ, L)
        x_hi = jnp.concatenate([a_all[p, 2, 0:3].reshape(NB, L), a_all[p, :, 3].reshape(NB, L)], axis=0)
        qg = dot(jnp.where(y == 0, x_lo, x_hi), wqg2[...])
        v2 = dot(x, wv2[...]).astype(BF16)
        kt = dot(wk2[...], x, 1, 1).astype(BF16)
        gate_sc[par] = jax.nn.sigmoid(qg[:, L:])
        q2 = (qg[:, :L] * (1.0 / math.sqrt(HD))).astype(BF16)
        for h in range(HEADS):
            vbd[par, h * NK:(h + 1) * NK, :] = jnp.where(hid == h, v2, jnp.zeros_like(v2))
        for t in range(2):
            q_sc[par, t, :, :C] = q2[:, t * C:(t + 1) * C]
            for h in range(HEADS):
                kbd[par, t, h * HD:(h + 1) * HD, h * NK:(h + 1) * NK] = kt[t * C + h * HD:t * C + (h + 1) * HD, :]

    for q in range(AHEAD):
        a_wait(q)
    for p in range(CHUNK * AHEAD):
        project(p, p)
    for u in range(2):
        bias_wait(u, across)
        fwd_copy(u).start()
    fill = down(jnp.where(mask_ref[...] > 0, 0.0, MASK_FILL).astype(F32), NK)
    for u in range(2):
        bias_wait(u, partner)
        bias_wait(u, cross)
        for g in range(3):
            parts = []
            for t in range(3):
                parts.append(bias_in[u, t, g].astype(F32) + fill[t * NB:(t + 1) * NB])
                parts.append(bias_in[u, 3, g, t * 32:(t + 1) * 32].astype(F32) + fill[3 * NB + t * 32:3 * NB + (t + 1) * 32])
            bt = jnp.transpose(jnp.concatenate(parts, axis=0)) * LOG2E
            bias_f[g, u * NB:(u + 1) * NB, :] = bt[:NB]
            bias_f[3, u * NB + g * 32:u * NB + (g + 1) * 32, :] = bt[NB:]

    def softmax(t, logits):
        sums = []
        for h in range(HEADS):
            lt = logits[:, h * NK:(h + 1) * NK] * LOG2E + bias_f[h]
            e = jnp.exp2(lt - jnp.max(lt, axis=1, keepdims=True))
            sums.append(jnp.sum(e, axis=1, keepdims=True))
            p_sc[t, :, h * NK:(h + 1) * NK] = e.astype(BF16)
        return sums

    def attend(p, par):
        logits = [dot(q_sc[par, t, :, :C], kbd[par, t]) for t in range(2)]
        sums = [softmax(t, logits[t]) for t in range(2)]
        o = []
        for t in range(2):
            l = sums[t]
            div = jnp.where(hid_q == 0, l[0], jnp.where(hid_q == 1, l[1], jnp.where(hid_q == 2, l[2], l[3])))
            o.append(dot(p_sc[t], vbd[par]) / div)
        res = gate_sc[par] * jnp.where(lane_q < C, o[0], o[1])
        gf[pl.ds(s * PAIRS + p, NB, stride=2 * PAIRS), :] = jnp.where(s == 0, res[:NB], res[NB:])
        g_send[p] = jnp.where(s == 0, res[NB:], res[:NB]).astype(BF16)

    def g_copy(q):
        return pltpu.make_async_remote_copy(
            src_ref=g_send.at[pl.ds(q * CHUNK, CHUNK)], dst_ref=g_recv.at[pl.ds(q * CHUNK, CHUNK)],
            send_sem=g_ssem.at[q], recv_sem=g_rsem.at[q], device_id={"row": partner}, device_id_type=MESH)

    for q in range(AHEAD):
        if q == AHEAD - 1:
            a_wait(AHEAD)
        for p in range(q * CHUNK, (q + 1) * CHUNK):
            if p == CHUNK * AHEAD - 1:
                project(p + 1, 0)
            attend(p, p)
        g_copy(q).start()

    @pl.loop(AHEAD, NCH)
    def _(q):
        p = q * CHUNK

        @pl.when(q < NCH - 1)
        def _():
            a_wait(q + 1)

        project(p + 1, 1)
        attend(p, 0)
        project(jnp.minimum(p + 2, PAIRS - 1), 0)
        attend(p + 1, 1)
        g_copy(q).start()

    for q in range(NCH):
        g_copy(q).wait_recv()

    @pl.loop(0, PAIRS, unroll=4)
    def _(p):
        gf[pl.ds((1 - s) * PAIRS + p, NB, stride=2 * PAIRS), :] = g_recv[p].astype(F32)

    @pl.loop(0, NB // 4, unroll=8)
    def _(i4):
        rows = pl.ds(pl.multiple_of(i4 * 192, 64), 192)
        out_ref[rows, :] = gf[rows, :].astype(BF16)

    for q in range(NCH):
        g_copy(q).wait_send()
        for slot in range(3):
            a_desc(slot, q, peers[slot], False).wait_send()
    for k in range(4):
        @pl.when(z_dest(k) != col)
        def _(k=k):
            z_copy(k).wait_send()
    for u in range(2):
        y_copy(u).wait_send()
        own_copy(u).wait_send()
        fwd_copy(u).wait_send()


def project_out(gated_ref, z_ref, wo_ref, out_ref):
    wo = wo_ref[...]
    zero = jnp.zeros_like(wo)
    swapped = jnp.concatenate([jnp.concatenate([zero, wo], 1), jnp.concatenate([wo, zero], 1)], 0)
    wo4 = jnp.concatenate([blockdiag2(wo), swapped], axis=1)
    lane_o = lax.broadcasted_iota(jnp.int32, (2 * PAIRS, L), 1)
    for i4 in range(STEP // 4):
        r4 = dot(gated_ref[i4 * 192:(i4 + 1) * 192, :], wo4)
        for k in range(2):
            ra, rb = r4[k * 96:k * 96 + 48], r4[k * 96 + 48:(k + 1) * 96]
            c0 = jnp.where(lane_o < C, ra[:, :L], rb[:, L:])
            c1 = jnp.where(lane_o < C, ra[:, L:], rb[:, :L])
            both = jnp.transpose(jnp.concatenate([c0[:PAIRS], c1[:PAIRS], c0[PAIRS:], c1[PAIRS:]], axis=0))
            i = i4 * 4 + 2 * k
            out_ref[i] = (z_ref[i].astype(F32) + both[:C]).astype(BF16)
            out_ref[i + 1] = (z_ref[i + 1].astype(F32) + both[C:]).astype(BF16)


def solution(mesh):
    vm = pl.BlockSpec(memory_space=pltpu.VMEM)
    dma = pltpu.SemaphoreType.DMA

    def body(pair_tile, res_mask, ln_gamma, ln_beta, w_q, w_k, w_v, w_b, w_g, w_o):
        z_t = jnp.transpose(pair_tile, (0, 2, 1))
        gated = pl.pallas_call(
            kernel,
            out_shape=jax.ShapeDtypeStruct((NB * 2 * PAIRS, L), BF16),
            in_specs=[vm] * 9,
            out_specs=vm,
            scratch_shapes=[
                pltpu.VMEM((NB * 2 * PAIRS, L), F32),
                pltpu.VMEM((NB, 8, L), F32),
                pltpu.VMEM((2 * PAIRS, 3, 32, L), BF16),
                pltpu.VMEM((PAIRS, 3, 4, 32, L), BF16),
                pltpu.VMEM((4, 3, NB, L), BF16),
                pltpu.VMEM((2, 4, 3, NB, L), BF16),
                pltpu.VMEM((HEADS, NQ, NK), F32),
                pltpu.VMEM((CHUNK * AHEAD, 2, C, HEADS * NK), BF16),
                pltpu.VMEM((CHUNK * AHEAD, HEADS * NK, L), BF16),
                pltpu.VMEM((CHUNK * AHEAD, 2, NQ, L), BF16),
                pltpu.VMEM((CHUNK * AHEAD, NQ, L), F32),
                pltpu.VMEM((2, NQ, HEADS * NK), BF16),
                pltpu.VMEM((PAIRS, NB, L), BF16),
                pltpu.VMEM((PAIRS, NB, L), BF16),
                pltpu.VMEM((NB * 2 * PAIRS, L), F32),
                pltpu.VMEM((L, L), BF16),
                pltpu.VMEM((L, L), BF16),
                pltpu.VMEM((L, 2 * L), BF16),
                dma((3, NCH)), dma((3, NCH)), dma((4,)), dma((4,)), dma((2,)), dma((2, 2)), dma((2, 4)),
                dma((NCH,)), dma((NCH,)),
            ],
            compiler_params=pltpu.CompilerParams(collective_id=0, has_side_effects=True, vmem_limit_bytes=56 * 2**20),
            name="attend",
        )(z_t, res_mask, ln_gamma, ln_beta, w_q, w_k, w_v, w_b.T, w_g)
        tile = pl.BlockSpec((STEP, C, NB), lambda n: (n, 0, 0))
        out = pl.pallas_call(
            project_out,
            out_shape=jax.ShapeDtypeStruct((NB, C, NB), BF16),
            grid=(NB // STEP,),
            in_specs=[pl.BlockSpec((STEP * 2 * PAIRS, L), lambda n: (n, 0)), tile, pl.BlockSpec((C, C), lambda n: (0, 0))],
            out_specs=tile,
            name="project_out",
        )(gated, z_t, w_o)
        return jnp.transpose(out, (0, 2, 1))

    tile_spec = P(("data", "row"), "col", None)
    return jax.shard_map(body, mesh=mesh, in_specs=(tile_spec, P("data"), P(), P(), P(), P(), P(), P(), P(), P()),
                         out_specs=tile_spec, check_vma=False)
```

```python
import math

import jax
import jax.numpy as jnp
from jax import lax
from jax.experimental import pallas as pl
from jax.experimental.pallas import tpu as pltpu
from jax.sharding import PartitionSpec as P

LN_EPS = 1e-5
MASK_FILL = -1e9
LOG2E = math.log2(math.e)
HEADS = 4
HD = 16
C = 64
NB = 96
NK = 384
NQ = 192
PAIRS = 24
CHUNK = 2
NCH = PAIRS // CHUNK
UNR = 24
STEP = 48
AHEAD = 2
L = 128
MESH = pl.DeviceIdType.MESH
F32 = jnp.float32
BF16 = jnp.bfloat16


def dot(a, b, ca=1, cb=0):
    return lax.dot_general(a, b, (((ca,), (cb,)), ((), ())), preferred_element_type=F32)


def blockdiag2(w):
    z = jnp.zeros_like(w)
    return jnp.concatenate([jnp.concatenate([w, z], 1), jnp.concatenate([z, w], 1)], 0)


def transposed(w):
    return jnp.transpose(w.astype(F32)).astype(BF16)


def down(v, n):
    return jnp.transpose(jnp.broadcast_to(v.reshape(1, n), (L, n)))


def kernel(z_ref, mask_ref, gam_ref, bet_ref, wq_ref, wk_ref, wv_ref, wbt_ref, wg_ref, out_ref,
           t_sc, b_sc, a_own, a_all, bias_z, bias_in, bias_f, kbd, vbd, q_sc, gate_sc, p_sc, g_send, g_recv, gf,
           wk2, wv2, wqg2,
           a_ssem, a_rsem, z_ssem, z_rsem, y_ssem, f_ssem, b_rsem, g_ssem, g_rsem):
    col = lax.axis_index("col")
    row = lax.axis_index("row")
    y, s = row // 2, lax.rem(row, 2)
    partner = y * 2 + (1 - s)
    across = (1 - y) * 2 + s
    cross = (1 - y) * 2 + (1 - s)
    peers = (partner, across, cross)

    barrier = pltpu.get_barrier_semaphore()
    for r in peers:
        pl.semaphore_signal(barrier, inc=1, device_id={"row": r}, device_id_type=MESH)
    for d in range(1, 4):
        pl.semaphore_signal(barrier, inc=1, device_id={"col": lax.rem(col + d, 4)}, device_id_type=MESH)

    gam = down(gam_ref[...], C)[:, :NB]
    bet = down(bet_ref[...], C)[:, :NB]
    wbt = wbt_ref[...]

    lane_t = lax.broadcasted_iota(jnp.int32, (PAIRS, L), 1)

    def normed(i):
        z = z_ref[i].astype(F32)
        mean = jnp.sum(z, axis=0, keepdims=True) * (1.0 / C)
        cen = z - mean
        var = jnp.sum(cen * cen, axis=0, keepdims=True) * (1.0 / C)
        a = cen * lax.rsqrt(var + LN_EPS) * gam + bet
        b_sc[i, :HEADS, :NB] = dot(wbt, a.astype(BF16))
        return a

    @pl.loop(0, NB // 2, unroll=UNR)
    def _(i2):
        at = jnp.transpose(jnp.concatenate([normed(2 * i2), normed(2 * i2 + 1)], axis=0))
        for half in range(2):
            o = half * 48
            lo, hi = at[o:o + PAIRS], at[o + PAIRS:o + 2 * PAIRS]
            base = pl.multiple_of(i2 * 96 + half * PAIRS, 8)
            t_sc[pl.ds(base, PAIRS), :] = jnp.where(lane_t < C, lo, pltpu.roll(hi, C, 1))
            t_sc[pl.ds(base + 48, PAIRS), :] = jnp.where(lane_t < C, pltpu.roll(lo, C, 1), hi)

    lane = lax.broadcasted_iota(jnp.int32, (NB, L), 1)
    bh = [b_sc.reshape(NB * 8, L)[pl.ds(h, NB, stride=8), :] for h in range(HEADS)]
    for g in range(3):
        bias_z[col, g] = jnp.where(lane < NB, bh[g], pltpu.roll(bh[3], NB - 32 * g, 1)).astype(BF16)

    pl.semaphore_wait(barrier, 6)

    def z_dest(k):
        return jnp.where(col < 2, 3 - k, k)

    def z_copy(k):
        return pltpu.make_async_remote_copy(
            src_ref=bias_z.at[col], dst_ref=bias_z.at[col], send_sem=z_ssem.at[k], recv_sem=z_rsem.at[col],
            device_id={"col": z_dest(k)}, device_id_type=MESH)

    def z_wait(c):
        pltpu.make_async_remote_copy(
            src_ref=bias_z.at[c], dst_ref=bias_z.at[c], send_sem=z_ssem.at[0], recv_sem=z_rsem.at[c],
            device_id={"col": lax.rem(col + 1, 4)}, device_id_type=MESH).wait_recv()

    def bias_copy(src, u, r, ssem, dev):
        return pltpu.make_async_remote_copy(
            src_ref=src, dst_ref=bias_in.at[u, r], send_sem=ssem, recv_sem=b_rsem.at[u, r],
            device_id={"row": dev}, device_id_type=MESH)

    def y_copy(u):
        return bias_copy(bias_z.at[2 * (1 - y) + u], u, row, y_ssem.at[u], across)

    def own_copy(u):
        return bias_copy(bias_z.at[2 * y + u], u, row, f_ssem.at[u, 0], partner)

    def fwd_copy(u):
        return bias_copy(bias_in.at[u, across], u, across, f_ssem.at[u, 1], partner)

    def bias_wait(u, r):
        bias_copy(bias_in.at[u, r], u, r, y_ssem.at[u], partner).wait_recv()

    for k in range(4):
        @pl.when(z_dest(k) != col)
        def _(k=k):
            z_copy(k).start()

    @pl.loop(0, 2 * PAIRS, unroll=8)
    def _(n):
        a_own[n] = t_sc[pl.ds(n, NB, stride=2 * PAIRS), :].astype(BF16).reshape(3, 32, L)

    def a_desc(slot, q, r, last):
        dst = a_all.at[pl.ds(q * CHUNK, CHUNK), :, 3] if last else a_all.at[pl.ds(q * CHUNK, CHUNK), jnp.minimum(row, 2), 0:3]
        return pltpu.make_async_remote_copy(
            src_ref=a_own.at[pl.ds(lax.rem(r, 2) * PAIRS + q * CHUNK, CHUNK)], dst_ref=dst,
            send_sem=a_ssem.at[slot, q], recv_sem=a_rsem.at[slot, q],
            device_id={"row": r}, device_id_type=MESH)

    def a_start(slot, q):
        @pl.when(row == 3)
        def _():
            a_desc(slot, q, peers[slot], True).start()

        @pl.when(row < 3)
        def _():
            a_desc(slot, q, peers[slot], False).start()

    for q in range(AHEAD):
        for slot in (1, 2, 0):
            a_start(slot, q)

    @pl.when(row == 3)
    def _():
        a_all[:, :, 3] = a_own[pl.ds(s * PAIRS, PAIRS)]

    @pl.when(row < 3)
    def _():
        a_all[:, jnp.minimum(row, 2), 0:3] = a_own[pl.ds(s * PAIRS, PAIRS)]

    wk2[...] = blockdiag2(transposed(wk_ref[...]))
    wv2[...] = blockdiag2(wv_ref[...])
    wqg2[:, :L] = blockdiag2(wq_ref[...])
    wqg2[:, L:] = blockdiag2(wg_ref[...])
    for par in range(CHUNK * AHEAD):
        for t in range(2):
            kbd[par, t] = jnp.zeros((C, HEADS * NK), BF16)

    for u in range(2):
        @pl.when(2 * (1 - y) + u != col)
        def _(u=u):
            z_wait(2 * (1 - y) + u)
        y_copy(u).start()
    for q in range(AHEAD, NCH):
        for slot in (1, 2, 0):
            a_start(slot, q)
    for u in range(2):
        @pl.when(2 * y + u != col)
        def _(u=u):
            z_wait(2 * y + u)
        own_copy(u).start()
        bias_in[u, row] = bias_z[2 * y + u]
    def a_wait(q):
        for slot in range(3):
            a_desc(slot, q, peers[slot], False).wait_recv()

    hid = lax.rem(lax.broadcasted_iota(jnp.int32, (NK, L), 1), C) // HD
    lane_q = lax.broadcasted_iota(jnp.int32, (NQ, L), 1)
    hid_q = lax.rem(lane_q, C) // HD

    def project(p, par):
        x = a_all[p].reshape(NK, L)
        x_lo = a_all[p, 0:2, 0:3].reshape(NQ, L)
        x_hi = jnp.concatenate([a_all[p, 2, 0:3].reshape(NB, L), a_all[p, :, 3].reshape(NB, L)], axis=0)
        qg = dot(jnp.where(y == 0, x_lo, x_hi), wqg2[...])
        v2 = dot(x, wv2[...]).astype(BF16)
        kt = dot(wk2[...], x, 1, 1).astype(BF16)
        gate_sc[par] = jax.nn.sigmoid(qg[:, L:])
        q2 = (qg[:, :L] * (1.0 / math.sqrt(HD))).astype(BF16)
        for h in range(HEADS):
            vbd[par, h * NK:(h + 1) * NK, :] = jnp.where(hid == h, v2, jnp.zeros_like(v2))
        for t in range(2):
            q_sc[par, t, :, :C] = q2[:, t * C:(t + 1) * C]
            for h in range(HEADS):
                kbd[par, t, h * HD:(h + 1) * HD, h * NK:(h + 1) * NK] = kt[t * C + h * HD:t * C + (h + 1) * HD, :]

    for q in range(AHEAD):
        a_wait(q)
    for p in range(CHUNK * AHEAD):
        project(p, p)
    for u in range(2):
        bias_wait(u, across)
        fwd_copy(u).start()
    fill = down(jnp.where(mask_ref[...] > 0, 0.0, MASK_FILL).astype(F32), NK)
    for u in range(2):
        bias_wait(u, partner)
        bias_wait(u, cross)
        for g in range(3):
            parts = []
            for t in range(3):
                parts.append(bias_in[u, t, g].astype(F32) + fill[t * NB:(t + 1) * NB])
                parts.append(bias_in[u, 3, g, t * 32:(t + 1) * 32].astype(F32) + fill[3 * NB + t * 32:3 * NB + (t + 1) * 32])
            bt = jnp.transpose(jnp.concatenate(parts, axis=0)) * LOG2E
            bias_f[g, u * NB:(u + 1) * NB, :] = bt[:NB]
            bias_f[3, u * NB + g * 32:u * NB + (g + 1) * 32, :] = bt[NB:]

    def softmax(t, logits):
        sums = []
        for h in range(HEADS):
            lt = logits[:, h * NK:(h + 1) * NK] * LOG2E + bias_f[h]
            e = jnp.exp2(lt - jnp.max(lt, axis=1, keepdims=True))
            sums.append(jnp.sum(e, axis=1, keepdims=True))
            p_sc[t, :, h * NK:(h + 1) * NK] = e.astype(BF16)
        return sums

    def attend(p, par):
        logits = [dot(q_sc[par, t, :, :C], kbd[par, t]) for t in range(2)]
        sums = [softmax(t, logits[t]) for t in range(2)]
        o = []
        for t in range(2):
            l = sums[t]
            div = jnp.where(hid_q == 0, l[0], jnp.where(hid_q == 1, l[1], jnp.where(hid_q == 2, l[2], l[3])))
            o.append(dot(p_sc[t], vbd[par]) / div)
        res = gate_sc[par] * jnp.where(lane_q < C, o[0], o[1])
        gf[pl.ds(s * PAIRS + p, NB, stride=2 * PAIRS), :] = jnp.where(s == 0, res[:NB], res[NB:])
        g_send[p] = jnp.where(s == 0, res[NB:], res[:NB]).astype(BF16)

    def g_copy(q):
        return pltpu.make_async_remote_copy(
            src_ref=g_send.at[pl.ds(q * CHUNK, CHUNK)], dst_ref=g_recv.at[pl.ds(q * CHUNK, CHUNK)],
            send_sem=g_ssem.at[q], recv_sem=g_rsem.at[q], device_id={"row": partner}, device_id_type=MESH)

    for q in range(AHEAD):
        if q == AHEAD - 1:
            a_wait(AHEAD)
        for p in range(q * CHUNK, (q + 1) * CHUNK):
            if p == CHUNK * AHEAD - 1:
                project(p + 1, 0)
            attend(p, p)
        g_copy(q).start()

    @pl.loop(AHEAD, NCH)
    def _(q):
        p = q * CHUNK

        @pl.when(q < NCH - 1)
        def _():
            a_wait(q + 1)

        project(p + 1, 1)
        attend(p, 0)
        project(jnp.minimum(p + 2, PAIRS - 1), 0)
        attend(p + 1, 1)
        g_copy(q).start()

    for q in range(NCH):
        g_copy(q).wait_recv()

    @pl.loop(0, PAIRS, unroll=4)
    def _(p):
        gf[pl.ds((1 - s) * PAIRS + p, NB, stride=2 * PAIRS), :] = g_recv[p].astype(F32)

    @pl.loop(0, NB // 4, unroll=8)
    def _(i4):
        rows = pl.ds(pl.multiple_of(i4 * 192, 64), 192)
        out_ref[rows, :] = gf[rows, :].astype(BF16)

    for q in range(NCH):
        g_copy(q).wait_send()
        for slot in range(3):
            a_desc(slot, q, peers[slot], False).wait_send()
    for k in range(4):
        @pl.when(z_dest(k) != col)
        def _(k=k):
            z_copy(k).wait_send()
    for u in range(2):
        y_copy(u).wait_send()
        own_copy(u).wait_send()
        fwd_copy(u).wait_send()


def project_out(gated_ref, z_ref, wo_ref, out_ref):
    wo = wo_ref[...]
    zero = jnp.zeros_like(wo)
    swapped = jnp.concatenate([jnp.concatenate([zero, wo], 1), jnp.concatenate([wo, zero], 1)], 0)
    wo4 = jnp.concatenate([blockdiag2(wo), swapped], axis=1)
    lane_o = lax.broadcasted_iota(jnp.int32, (2 * PAIRS, L), 1)
    for i4 in range(STEP // 4):
        r4 = dot(gated_ref[i4 * 192:(i4 + 1) * 192, :], wo4)
        for k in range(2):
            ra, rb = r4[k * 96:k * 96 + 48], r4[k * 96 + 48:(k + 1) * 96]
            c0 = jnp.where(lane_o < C, ra[:, :L], rb[:, L:])
            c1 = jnp.where(lane_o < C, ra[:, L:], rb[:, :L])
            both = jnp.transpose(jnp.concatenate([c0[:PAIRS], c1[:PAIRS], c0[PAIRS:], c1[PAIRS:]], axis=0))
            i = i4 * 4 + 2 * k
            out_ref[i] = (z_ref[i].astype(F32) + both[:C]).astype(BF16)
            out_ref[i + 1] = (z_ref[i + 1].astype(F32) + both[C:]).astype(BF16)


def solution(mesh):
    vm = pl.BlockSpec(memory_space=pltpu.VMEM)
    dma = pltpu.SemaphoreType.DMA

    def body(pair_tile, res_mask, ln_gamma, ln_beta, w_q, w_k, w_v, w_b, w_g, w_o):
        z_t = jnp.transpose(pair_tile, (0, 2, 1))
        gated = pl.pallas_call(
            kernel,
            out_shape=jax.ShapeDtypeStruct((NB * 2 * PAIRS, L), BF16),
            in_specs=[vm] * 9,
            out_specs=vm,
            scratch_shapes=[
                pltpu.VMEM((NB * 2 * PAIRS, L), F32),
                pltpu.VMEM((NB, 8, L), F32),
                pltpu.VMEM((2 * PAIRS, 3, 32, L), BF16),
                pltpu.VMEM((PAIRS, 3, 4, 32, L), BF16),
                pltpu.VMEM((4, 3, NB, L), BF16),
                pltpu.VMEM((2, 4, 3, NB, L), BF16),
                pltpu.VMEM((HEADS, NQ, NK), F32),
                pltpu.VMEM((CHUNK * AHEAD, 2, C, HEADS * NK), BF16),
                pltpu.VMEM((CHUNK * AHEAD, HEADS * NK, L), BF16),
                pltpu.VMEM((CHUNK * AHEAD, 2, NQ, L), BF16),
                pltpu.VMEM((CHUNK * AHEAD, NQ, L), F32),
                pltpu.VMEM((2, NQ, HEADS * NK), BF16),
                pltpu.VMEM((PAIRS, NB, L), BF16),
                pltpu.VMEM((PAIRS, NB, L), BF16),
                pltpu.VMEM((NB * 2 * PAIRS, L), F32),
                pltpu.VMEM((L, L), BF16),
                pltpu.VMEM((L, L), BF16),
                pltpu.VMEM((L, 2 * L), BF16),
                dma((3, NCH)), dma((3, NCH)), dma((4,)), dma((4,)), dma((2,)), dma((2, 2)), dma((2, 4)),
                dma((NCH,)), dma((NCH,)),
            ],
            compiler_params=pltpu.CompilerParams(collective_id=0, has_side_effects=True, vmem_limit_bytes=56 * 2**20),
            name="attend",
        )(z_t, res_mask, ln_gamma, ln_beta, w_q, w_k, w_v, w_b.T, w_g)
        tile = pl.BlockSpec((STEP, C, NB), lambda n: (n, 0, 0))
        out = pl.pallas_call(
            project_out,
            out_shape=jax.ShapeDtypeStruct((NB, C, NB), BF16),
            grid=(NB // STEP,),
            in_specs=[pl.BlockSpec((STEP * 2 * PAIRS, L), lambda n: (n, 0)), tile, pl.BlockSpec((C, C), lambda n: (0, 0))],
            out_specs=tile,
            name="project_out",
        )(gated, z_t, w_o)
        return jnp.transpose(out, (0, 2, 1))

    tile_spec = P(("data", "row"), "col", None)
    return jax.shard_map(body, mesh=mesh, in_specs=(tile_spec, P("data"), P(), P(), P(), P(), P(), P(), P(), P()),
                         out_specs=tile_spec, check_vma=False)
```
